32 devices in a mesh: row: 8 (over y, x, core), col: 4 (over z).
Axes of the slice: x: 2, y: 2, z: 4, core: 2. Of those that a mesh axis runs over, the one named last changes fastest.
Arguments:
- slc_stack: float32 [20, 2, 64, 512], P(None, None, 'row', 'col'), may hold values from -6 to 6
- land_mask: int32 [64, 512], P('row', 'col'), may hold values from 0 to 1, as said below
Outputs:
- linked: float32 [20, 2, 64, 512], P(None, None, 'row', 'col')
- compressed_final: float32 [2, 64, 512], P(None, 'row', 'col')
- mean_strength: float32 [2], replicated
The draws below stay inside these ranges and needn't reach their ends.
Inputs may be any that keep to these rules, and one draw needn't show every extreme that they name: `land_mask`: 1 marks a valid pixel, 0 a water pixel.
All inputs are finite; a program needn't handle non-finite values.
Results may differ from the reference program's by a relative error of at most 0.00012.
Values sent between devices are 32-bit elements; how exact they have to be, the bound alone decides.
A program may use at most 64 MiB of HBM per device.

```python
import jax
import jax.numpy as jnp
import numpy as np
from jax import lax

M = 10
MS = 2
WIN = 11
ITERS = 4
CR = 8
NR = 64
NC = 512
DATES = 20


def draw_land_mask(key, part):
    tile_rows = NR // 16 + 2
    tile_cols = NC // 16 + 2
    offset_key, tile_key = jax.random.split(jax.random.fold_in(key, 11))
    offsets = jax.random.randint(offset_key, (2,), 0, 16)
    row_level = 33 + 67 * jnp.arange(tile_rows, dtype=jnp.int32) // (tile_rows - 1)
    col_level = 33 + 67 * jnp.arange(tile_cols, dtype=jnp.int32) // (tile_cols - 1)
    chance = row_level[:, None] * col_level[None, :]
    samples = jax.random.randint(tile_key, (tile_rows, tile_cols), 0, 10000)
    tiles = (samples < chance).astype(jnp.int32)
    row_tile = (jnp.arange(NR, dtype=jnp.int32) + offsets[0]) // 16
    col_tile = (jnp.arange(NC, dtype=jnp.int32) + offsets[1]) // 16
    return tiles[row_tile][:, col_tile]


def block_scale(stream_key, extent, cuts, smallest, largest):
    def one(position, blocks):
        draws = jax.random.uniform(jax.random.fold_in(jax.random.fold_in(stream_key, 6), position), (blocks,), jnp.float32, smallest / len(cuts), largest / len(cuts))
        return jnp.repeat(jnp.exp(draws), extent[position] // blocks).reshape((-1,) + (1,) * (len(extent) - position - 1))

    loudness = one(*cuts[0])
    for cut in cuts[1:]:
        loudness = loudness * one(*cut)
    return loudness


def gaussian(own_key, dims, scale, most, cuts=(), held_as=jnp.bfloat16):
    values = jax.random.normal(own_key, dims, jnp.float32) * scale
    if len(cuts) > 0:
        values = block_scale(own_key, dims, cuts, -0.22, 0.18) * values
    return jnp.clip(values, min=-most, max=most).astype(held_as)


def setup_inputs(seed: int = 0) -> dict:
    streams_of = jax.random.split(jax.random.key(seed), 3)
    slc_stack = gaussian(streams_of[0], (DATES, 2, NR, NC), 1.0, 6.0, ((2, 8), (3, 4)), jnp.float32)
    land_mask = draw_land_mask(jax.random.fold_in(streams_of[2], 71), 0)
    return dict(slc_stack=slc_stack, land_mask=land_mask)


covariance_floor = 8.0

def pair_tables(number):
    upper_first, upper_second = np.triu_indices(number)
    strict_first, strict_second = np.triu_indices(number, 1)
    real_slot = np.zeros((number, number), np.int32)
    real_slot[upper_first, upper_second] = np.arange(upper_first.size)
    real_slot[upper_second, upper_first] = np.arange(upper_first.size)
    base_slot = upper_first.size
    imag_slot = np.full((number, number), base_slot + strict_first.size, np.int32)
    imag_sign = np.zeros((number, number), np.float32)
    imag_slot[strict_first, strict_second] = base_slot + np.arange(strict_first.size)
    imag_slot[strict_second, strict_first] = base_slot + np.arange(strict_first.size)
    imag_sign[strict_first, strict_second] = 1.0
    imag_sign[strict_second, strict_first] = -1.0
    return (upper_first, upper_second, strict_first, strict_second, real_slot.reshape(-1), imag_slot.reshape(-1), imag_sign.reshape(-1))

def pair_products(padded, tables):
    upper_first, upper_second, strict_first, strict_second = (tables[0], tables[1], tables[2], tables[3])
    left_upper = padded[upper_first]
    right_upper = padded[upper_second]
    real_fields = left_upper[:, 0] * right_upper[:, 0] + left_upper[:, 1] * right_upper[:, 1]
    left_strict = padded[strict_first]
    right_strict = padded[strict_second]
    imag_fields = left_strict[:, 1] * right_strict[:, 0] - left_strict[:, 0] * right_strict[:, 1]
    return jnp.concatenate([real_fields, imag_fields], 0)

def box_sum(products, height, width, reach):
    along_rows = products[:, 0:height, :]
    for offset in range(1, 2 * reach + 1):
        along_rows = along_rows + products[:, offset:offset + height, :]
    windowed = along_rows[:, :, 0:width]
    for offset in range(1, 2 * reach + 1):
        windowed = windowed + along_rows[:, :, offset:offset + width]
    return windowed

def finish(windowed, fresh, land_float, number, tables):
    real_slot, imag_slot, imag_sign = (tables[4], tables[5], tables[6])
    shape_tail = windowed.shape[1:]
    extended = jnp.concatenate([windowed, jnp.zeros_like(windowed[:1])], 0)
    cov_real = windowed[real_slot].reshape((number, number) + shape_tail)
    cov_imag = (extended[imag_slot] * imag_sign[:, None, None]).reshape((number, number) + shape_tail)
    diagonal = windowed[real_slot[::number + 1]]
    scales = 1.0 / jnp.sqrt(jnp.maximum(diagonal, covariance_floor))
    coh_real = cov_real * scales[:, None] * scales[None, :]
    coh_imag = cov_imag * scales[:, None] * scales[None, :]
    vec_real = jnp.ones((number,) + shape_tail, jnp.float32)
    vec_imag = jnp.zeros((number,) + shape_tail, jnp.float32)
    length = jnp.zeros(shape_tail, jnp.float32)
    for iteration in range(ITERS):
        next_real = lax.optimization_barrier(jnp.sum(coh_real * vec_real[None] - coh_imag * vec_imag[None], axis=1))
        next_imag = lax.optimization_barrier(jnp.sum(coh_real * vec_imag[None] + coh_imag * vec_real[None], axis=1))
        length = jnp.sqrt(lax.optimization_barrier(jnp.sum(next_real * next_real + next_imag * next_imag, axis=0)))
        divisor = jnp.maximum(length, 1.0)
        vec_real = next_real / divisor
        vec_imag = next_imag / divisor
    strength = jnp.sum(land_float * length) / number
    new_real = vec_real[number - M:]
    new_imag = vec_imag[number - M:]
    comp_real = lax.optimization_barrier(jnp.sum(new_real * fresh[:, 0] + new_imag * fresh[:, 1], axis=0))
    comp_imag = lax.optimization_barrier(jnp.sum(new_real * fresh[:, 1] - new_imag * fresh[:, 0], axis=0))
    linked_part = jnp.stack([new_real, new_imag], 1) * land_float
    compressed = jnp.stack([comp_real, comp_imag], 0)[None]
    return (linked_part, compressed, strength)

def reference(slc_stack, land_mask):
    reach = WIN // 2
    land_float = land_mask.astype(jnp.float32)
    signal = slc_stack * land_float
    strip_count = NR // CR
    carried_list = []
    linked_parts = []
    totals = []
    compressed = None
    for ministack in range(MS):
        number = ministack + M
        tables = pair_tables(number)
        fresh = signal[ministack * M:(ministack + 1) * M]
        stacked = jnp.concatenate(carried_list + [fresh], 0)
        padded = jnp.pad(stacked, ((0, 0), (0, 0), (reach, reach), (reach, reach)))

        def strip_work(strip_index, padded=padded, fresh=fresh, number=number, tables=tables):
            top = strip_index * CR
            block = lax.dynamic_slice_in_dim(padded, top, CR + 2 * reach, 2)
            fresh_block = lax.dynamic_slice_in_dim(fresh, top, CR, 2)
            land_block = lax.dynamic_slice_in_dim(land_float, top, CR, 0)
            products = pair_products(block, tables)
            windowed = box_sum(products, CR, NC, reach)
            return finish(windowed, fresh_block, land_block, number, tables)
        linked_strips, comp_strips, strength_strips = lax.map(strip_work, jnp.arange(strip_count, dtype=jnp.int32))
        linked_parts.append(jnp.transpose(linked_strips, (1, 2, 0, 3, 4)).reshape(M, 2, NR, NC))
        compressed = jnp.transpose(comp_strips, (1, 2, 0, 3, 4)).reshape(1, 2, NR, NC)
        carried_list.append(compressed)
        totals.append(jnp.sum(strength_strips))
    mean_strength = jnp.stack(totals) / (NR * NC)
    return (jnp.concatenate(linked_parts, 0), compressed[0], mean_strength)
```

```python
import functools

import jax
import jax.numpy as jnp
from jax import lax
from jax.experimental import pallas as pl
from jax.experimental.pallas import tpu as pltpu
from jax.sharding import PartitionSpec as P

M = 10
MS = 2
WIN = 11
ITERS = 4
REACH = WIN // 2
SUB = 8

covariance_floor = 8.0

AROUND = ((-1, 0), (1, 0), (-1, -1), (0, -1), (1, -1), (-1, 1), (0, 1), (1, 1))
LINE = 2 * M
EDGE = -(-REACH * LINE // SUB) * SUB
SKIP = EDGE - REACH * LINE
PACK = -(-LINE // SUB) * SUB


def pair_groups():
    groups = [[(s, (s + lag) % SUB) for s in range(SUB)] for lag in range(1, SUB // 2)]
    half = SUB // 2
    groups.append([(s, s + half) for s in range(half)] + [(M - 2, M - 1), (M - 2, M - 2), (M - 1, M - 1)])
    groups.append([(s, M - 2) for s in range(SUB)])
    groups.append([(s, M - 1) for s in range(SUB)])
    groups.append([(s, s) for s in range(SUB)])
    return groups


def field_rows(groups):
    table = {}
    for unit, group in enumerate(groups):
        for lane, (i, j) in enumerate(group):
            for part in range(1 if i == j else 2):
                table[(i, j, part)] = unit * 2 * SUB + part * SUB + lane
    return table


GROUPS = pair_groups()
LATE = [[(s, M) for s in range(SUB)], [(M, M)] * (2 * SUB - M) + [(s, M) for s in range(SUB, M)]]
FIELDS = field_rows(GROUPS)
LATE_FIELDS = field_rows(LATE)
PAIRS = [(i, j) for i, j, part in FIELDS if part == 1]
LATE_PAIRS = [(i, j) for i, j, part in LATE_FIELDS if part == 1]
FRESH_ROWS = len(GROUPS) * 2 * SUB
LATE_ROWS = len(LATE) * 2 * SUB
FRESH_STEP = FRESH_ROWS + 4
LATE_STEP = LATE_ROWS + 4
SLOTS = 3 * (len(PAIRS) + len(LATE_PAIRS)) + M + 1


def window_sums(lines, outputs):
    core = lines[outputs - 1]
    for e in range(outputs, WIN):
        core = core + lines[e]
    low = [None] * outputs
    low[outputs - 1] = core
    for r in range(outputs - 2, -1, -1):
        low[r] = low[r + 1] + lines[r]
    sums = [low[0]]
    high = None
    for r in range(1, outputs):
        extra = lines[WIN - 1 + r]
        high = extra if high is None else high + extra
        sums.append(low[r] + high)
    return sums


def split(value):
    high = value.astype(jnp.bfloat16)
    low = (value - high.astype(jnp.float32)).astype(jnp.bfloat16)
    return high, low


def waves(row_count, col_count):
    offsets = []
    known = 1
    while known < max(row_count, col_count) - 1:
        offsets.append(known)
        known *= 2
    return offsets


def kernel(
    row_count,
    col_count,
    direct,
    slc_hbm,
    land_hbm,
    linked,
    comp_out,
    strength,
    slc,
    land,
    own,
    up,
    dn,
    pack_send,
    pack_recv,
    halo,
    comp_send,
    comp_up,
    comp_dn,
    cpack_send,
    cpack_recv,
    chalo,
    w_main,
    w_halo,
    ybuf,
    hbuf,
    ebuf,
    zbuf,
    zcbuf,
    coh,
    part,
    red_row,
    red_col,
    load_sem,
    ready,
    send_a,
    recv_a,
    send_b,
    recv_b,
    send_r,
    recv_r,
    send_c,
    recv_c,
):
    rows, cols = land.shape
    my_row = lax.axis_index("row")
    my_col = lax.axis_index("col")
    strip = rows * REACH
    mesh_id = pl.DeviceIdType.MESH
    loads = [
        pltpu.make_async_copy(slc_hbm, slc, load_sem.at[0]),
        pltpu.make_async_copy(land_hbm, land, load_sem.at[1]),
    ]
    for load in loads:
        load.start()

    def existing(dr, dc, far=1):
        ok = None
        for pos, step, count in ((my_row, dr, row_count), (my_col, dc, col_count)):
            if step:
                here = (pos >= far) if step < 0 else (pos < count - far)
                ok = here if ok is None else jnp.logical_and(ok, here)
        return ok

    exists = [existing(dr, dc) for dr, dc in AROUND]

    def greet(semaphore, far):
        expected = jnp.int32(0)
        for k, (dr, dc) in enumerate(AROUND):
            if (dr and far >= row_count) or (dc and far >= col_count):
                continue
            there = existing(dr, dc, far)

            @pl.when(there)
            def _(dr=dr, dc=dc):
                pl.semaphore_signal(
                    semaphore,
                    inc=1,
                    device_id=(my_row + dr * far, my_col + dc * far),
                    device_id_type=mesh_id,
                )

            expected = expected + there.astype(jnp.int32)
        return expected

    barrier = pltpu.get_barrier_semaphore()
    expected = greet(barrier, 1)
    offsets = waves(row_count, col_count)
    pending = []

    def next_wave():
        if pending:
            index, count = pending.pop()
            pl.semaphore_wait(ready.at[index], count)
            index += 1
        else:
            index = 0
        if index < len(offsets):
            pending.append((index, greet(ready.at[index], offsets[index])))

    for k, (dr, dc) in enumerate(AROUND):

        @pl.when(jnp.logical_not(exists[k]))
        def _(k=k, dc=dc, dr=dr):
            if dc == 0:
                target, small = (up, comp_up) if dr < 0 else (dn, comp_dn)
                for m in range(MS):
                    target[m] = jnp.zeros(target.shape[1:], jnp.float32)
                small[...] = jnp.zeros_like(small)
            else:
                for m in range(MS):
                    pack_recv[m, k - 2] = jnp.zeros(pack_recv.shape[2:], jnp.float32)
                cpack_recv[k - 2] = jnp.zeros(cpack_recv.shape[1:], jnp.float32)

    lane = lax.broadcasted_iota(jnp.int32, (rows, cols), 1)
    sub = lax.broadcasted_iota(jnp.int32, (rows, cols), 0)

    for load in loads:
        load.wait()
    mask = land[...].astype(jnp.float32)

    def place(m):
        for i in range(M):
            for c in range(2):
                own[m, pl.ds(c * M + i, rows, stride=LINE), :] = slc[m * M + i, c] * mask
        own[m, rows * LINE :, :] = jnp.zeros((own.shape[1] - rows * LINE, cols), jnp.float32)

    def spread(line, shift):
        total = pltpu.roll(line, cols - shift, 1) if shift else line
        return (
            total
            + pltpu.roll(line, (strip - shift) % cols, 1)
            + pltpu.roll(line, (2 * strip - shift) % cols, 1)
        )

    def pack(m):
        for at in range(0, PACK, SUB):
            low = high = jnp.zeros((SUB, cols), jnp.float32)
            for r in range(rows):
                turned = pltpu.roll(own[m, r * LINE + at : r * LINE + at + SUB, :], REACH * (r + 1), 1)
                high = jnp.where((lane >= r * REACH) & (lane < (r + 1) * REACH), turned, high)
                low = jnp.where((lane >= (r + 1) * REACH) & (lane < (r + 2) * REACH), turned, low)
            pack_send[m, 0, at : at + SUB, :] = spread(low, REACH)
            pack_send[m, 1, at : at + SUB, :] = spread(high, 0)

    def mirror(k):
        dr, dc = AROUND[k]
        return AROUND.index((-dr, -dc))

    def fresh_pair(m, k, sending):
        dr, dc = AROUND[k]
        back = mirror(k)
        slot = back if sending else k
        if dc == 0:
            source = own.at[m, pl.ds(0 if dr < 0 else rows * LINE - EDGE, EDGE)]
            target = (up if AROUND[slot][0] < 0 else dn).at[m, pl.ds(0, EDGE)]
        else:
            source = pack_send.at[m, 0 if dc < 0 else 1]
            target = pack_recv.at[m, slot - 2]
        return pltpu.make_async_remote_copy(
            src_ref=source,
            dst_ref=target,
            send_sem=send_a.at[m, k],
            recv_sem=recv_a.at[m, slot],
            device_id=(my_row + dr, my_col + dc),
            device_id_type=mesh_id,
        )

    def each_around(action):
        for k in range(len(AROUND)):

            @pl.when(exists[k])
            def _(k=k):
                action(k)

    place(0)
    pack(0)
    pl.semaphore_wait(barrier, expected)
    each_around(lambda k: fresh_pair(0, k, True).start())
    for m in range(1, MS):
        place(m)
        pack(m)
        each_around(lambda k, m=m: fresh_pair(m, k, True).start())
    next_wave()

    k_at = lax.broadcasted_iota(jnp.int32, (cols, cols), 0)
    n_at = lax.broadcasted_iota(jnp.int32, (cols, cols), 1)
    near = jnp.where((k_at - n_at <= REACH) & (n_at - k_at <= REACH), 1.0, 0.0).astype(jnp.bfloat16)
    w_main[0:cols, :] = near
    w_main[cols:, :] = near
    line_of = k_at // REACH
    inner = k_at - line_of * REACH
    for side in range(2):
        touches = (n_at <= inner) if side == 0 else (n_at >= inner + cols - REACH)
        line = jnp.where(touches, line_of, -1)
        for r in range(rows):
            first = rows - REACH + r
            w_halo[side * cols : (side + 1) * cols, r * cols : (r + 1) * cols] = jnp.where(
                (line >= first) & (line < first + WIN), 1.0, 0.0
            ).astype(jnp.bfloat16)

    lines_total = WIN + rows - 1

    def gather_halo(parts):
        sides = []
        for side in range(2):
            a, b, c = (parts(side * 3 + j) for j in range(3))
            which = lax.broadcasted_iota(jnp.int32, a.shape, 1)
            sides.append(jnp.where(which < strip, a, jnp.where(which < 2 * strip, b, c)))
        return sides

    def line_tile(m, e, c, first):
        if e < REACH:
            buffer, at = up, SKIP + e * LINE
        elif e < REACH + rows:
            buffer, at = own, (e - REACH) * LINE
        else:
            buffer, at = dn, (e - REACH - rows) * LINE
        at += c * M + first
        return buffer[m, at : at + SUB, :]

    def halo_tile(m, side, c, first):
        at = c * M + first
        return halo[m, side, at : at + SUB, :]

    def real_part(a, b, x, y):
        return a * x + b * y

    def imag_part(a, b, x, y):
        return b * x - a * y

    def operands(tile, unit):
        lead = [tile(c, 0) for c in range(2)]
        if unit < SUB // 2 - 1:
            return lead, [pltpu.roll(v, SUB - 1 - unit, 0) for v in lead]
        if unit == SUB // 2 - 1:
            left, right = [], []
            for c in range(2):
                mid, late = tile(c, SUB // 2), tile(c, SUB - M + 5)
                left.append(jnp.where(sub < 4, lead[c], jnp.where(sub == 4, mid, late)))
                right.append(jnp.where(sub < 4, mid, jnp.where(sub == 4, tile(c, 5), late)))
            return left, right
        return lead, None

    def products(tile, row_tile, unit):
        (a, b), other = operands(tile, unit)
        if unit == len(GROUPS) - 1:
            return a * a + b * b, None
        if other is None:
            image = M - 2 + unit - SUB // 2
            x, y = (jnp.broadcast_to(row_tile(c, image), (SUB, cols)) for c in range(2))
        else:
            x, y = other
        return real_part(a, b, x, y), imag_part(a, b, x, y)

    def tile_of(m, e):
        if e < lines_total:
            return functools.partial(line_tile, m, e)
        return functools.partial(halo_tile, m, e - lines_total)

    def row_of(m, e):
        tile = tile_of(m, e)
        return lambda c, image: tile(c, image)[0:1]

    def emit_side(unit, side, value):
        high, low = split(value)
        at = slice(unit * 2 * SUB, (unit + 1) * 2 * SUB)
        hbuf[0, at, side * cols : (side + 1) * cols] = high
        hbuf[1, at, side * cols : (side + 1) * cols] = low

    def edges(count):
        for r in range(0, rows, 2):
            band = w_halo[:, r * cols : (r + 2) * cols]
            value = jnp.dot(hbuf[0, 0:count], band, preferred_element_type=jnp.float32) + jnp.dot(
                hbuf[1, 0:count], band, preferred_element_type=jnp.float32
            )
            ebuf[r, 0:count] = value[:, 0:cols]
            ebuf[r + 1, 0:count] = value[:, cols:]

    def emit_lines(unit, lines, target, step):
        for r, total in enumerate(window_sums(lines, rows)):
            high, low = split(total)
            ybuf[unit, r * 2 * SUB : (r + 1) * 2 * SUB, 0:cols] = high
            ybuf[unit, r * 2 * SUB : (r + 1) * 2 * SUB, cols:] = low
        main = jnp.dot(ybuf[unit], w_main[...], preferred_element_type=jnp.float32)
        for r in range(rows):
            at = r * step + unit * 2 * SUB
            target[at : at + 2 * SUB, :] = (
                main[r * 2 * SUB : (r + 1) * 2 * SUB, :] + ebuf[r, unit * 2 * SUB : (unit + 1) * 2 * SUB]
            )

    def both_halves(pair):
        first, second = pair
        return jnp.concatenate([first, jnp.zeros_like(first) if second is None else second], 0)

    def fresh_fields(m):
        for side in range(2):
            for unit in range(len(GROUPS)):
                e = lines_total + side
                emit_side(unit, side, both_halves(products(tile_of(m, e), row_of(m, e), unit)))
        edges(FRESH_ROWS)
        for unit in range(len(GROUPS)):
            lines = [both_halves(products(tile_of(m, e), row_of(m, e), unit)) for e in range(lines_total)]
            emit_lines(unit, lines, zbuf, FRESH_STEP)

    def comp_row(e, c):
        if e < REACH:
            at = c * rows + rows - REACH + e
            return comp_up[at : at + 1, :]
        if e < REACH + rows:
            at = c * rows + e - REACH
            return comp_send[at : at + 1, :]
        if e < lines_total:
            at = c * rows + e - REACH - rows
            return comp_dn[at : at + 1, :]
        return chalo[e - lines_total, c : c + 1, :]

    def late_products(m, e, unit):
        tile = tile_of(m, e)
        x, y = (jnp.broadcast_to(comp_row(e, c), (SUB, cols)) for c in range(2))
        if unit == 0:
            a, b = tile(0, 0), tile(1, 0)
        else:
            a, b = (jnp.where(sub < 2 * SUB - M, v, tile(c, M - SUB)) for c, v in enumerate((x, y)))
        return jnp.concatenate([real_part(a, b, x, y), imag_part(a, b, x, y)], 0)

    def late_fields(m):
        for side in range(2):
            for unit in range(len(LATE)):
                emit_side(unit, side, late_products(m, lines_total + side, unit))
        edges(LATE_ROWS)
        for unit in range(len(LATE)):
            lines = [late_products(m, e, unit) for e in range(lines_total)]
            emit_lines(unit, lines, zcbuf, LATE_STEP)

    def fresh_field(i, j, p):
        return zbuf[pl.ds(FIELDS[(i, j, p)], rows, stride=FRESH_STEP), :]

    def late_field(i, j, p):
        return zcbuf[pl.ds(LATE_FIELDS[(i, j, p)], rows, stride=LATE_STEP), :]

    class Coherence:
        def __init__(self):
            self.scales = {}
            self.slot = {}
            self.re = {}
            self.im = {}
            self.used = 0

        def keep(self, key, value):
            coh[self.used] = value
            self.slot[key] = self.used
            self.used += 1

        def get(self, key):
            return coh[self.slot[key]]

        def tally(self, sums, i, value, minus=False):
            if i in sums:
                sums[i] = sums[i] - value if minus else sums[i] + value
            else:
                sums[i] = -value if minus else value

        def add(self, images, pairs, field):
            for i in images:
                value = field(i, i, 0)
                scale = lax.rsqrt(jnp.maximum(value, covariance_floor))
                self.scales[i] = scale
                value = value * (scale * scale)
                self.keep((i, i), value)
                self.tally(self.re, i, value)
            for i, j in pairs:
                s = self.scales[i] * self.scales[j]
                c = field(i, j, 0) * s
                d = field(i, j, 1) * s
                self.keep((i, j, 0), c)
                self.keep((i, j, 1), c + d)
                self.keep((i, j, 2), c - d)
                self.tally(self.re, i, c)
                self.tally(self.re, j, c)
                self.tally(self.im, i, d)
                self.tally(self.im, j, d, True)

        def power(self):
            images = sorted(self.re)
            re = [self.re[i] for i in images]
            im = [self.im[i] for i in images]
            gain = None
            for step in range(ITERS):
                if step:
                    both = [x + y for x, y in zip(re, im)]
                    new_re, new_im = [], []
                    for i in images:
                        shared = first = second = None
                        for j in images:
                            if j == i:
                                continue
                            key = (i, j) if (i, j, 0) in self.slot else (j, i)
                            turn = key != (i, j)
                            c = self.get(key + (0,)) * both[j]
                            e = self.get(key + (2 if turn else 1,)) * im[j]
                            f = self.get(key + (1 if turn else 2,)) * re[j]
                            shared = c if shared is None else shared + c
                            first = e if first is None else first + e
                            second = f if second is None else second + f
                        c = self.get((i, i))
                        new_re.append((shared - first) + c * re[i])
                        new_im.append((shared - second) + c * im[i])
                    re, im = new_re, new_im
                squares = [x * x + y * y for x, y in zip(re, im)]
                while len(squares) > 1:
                    squares = [sum(squares[k + 1 : k + 2], squares[k]) for k in range(0, len(squares), 2)]
                length = jnp.sqrt(squares[0])
                if gain is not None:
                    length = length * gain
                inverse = 1.0 / jnp.maximum(length, 1.0)
                gain = inverse if gain is None else gain * inverse
            return length, gain, re, im

    def finish(m, number, length, gain, re, im):
        comp_re = comp_im = None
        for i in range(M):
            a = own[m, pl.ds(i, rows, stride=LINE), :]
            b = own[m, pl.ds(M + i, rows, stride=LINE), :]
            x = re[i] * a + im[i] * b
            y = re[i] * b - im[i] * a
            comp_re = x if comp_re is None else comp_re + x
            comp_im = y if comp_im is None else comp_im + y
        return comp_re * gain, comp_im * gain

    def put_linked(m, gain, re, im):
        factor = gain * mask
        for i in range(M):
            linked[m * M + i, 0] = re[i] * factor
            linked[m * M + i, 1] = im[i] * factor

    def share_of(number, length):
        share = jnp.sum(mask * length, axis=0, keepdims=True) * (1.0 / number)
        return share + pltpu.roll(share, cols // 2, 1)

    def take_fresh(m):
        each_around(lambda k: fresh_pair(m, k, False).wait_recv())
        for side, value in enumerate(gather_halo(lambda j: pack_recv[m, j])):
            halo[m, side] = value

    take_fresh(0)
    next_wave()
    fresh_fields(0)
    early = Coherence()
    early.add(range(M), PAIRS, fresh_field)
    length, gain, re, im = early.power()
    comp_re, comp_im = finish(0, M, length, gain, re, im)
    comp_send[0:rows, :] = comp_re
    comp_send[rows:, :] = comp_im
    cpack_send[...] = jnp.zeros_like(cpack_send)
    for c, value in enumerate((comp_re, comp_im)):
        for side in range(2):
            total = jnp.zeros((rows, cols), jnp.float32)
            for copy in range(3):
                turned = pltpu.roll(value, REACH * side + strip * copy, 1, stride=REACH, stride_axis=0)
                first = strip * copy + sub * REACH
                total = jnp.where((lane >= first) & (lane < first + REACH), turned, total)
            cpack_send[side, c : c + 1, :] = jnp.sum(total, axis=0, keepdims=True)

    def comp_pair(k, sending):
        dr, dc = AROUND[k]
        slot = mirror(k) if sending else k
        if dc == 0:
            source = comp_send
            target = comp_up if AROUND[slot][0] < 0 else comp_dn
        else:
            source = cpack_send.at[0 if dc < 0 else 1]
            target = cpack_recv.at[slot - 2]
        return pltpu.make_async_remote_copy(
            src_ref=source,
            dst_ref=target,
            send_sem=send_b.at[k],
            recv_sem=recv_b.at[slot],
            device_id=(my_row + dr, my_col + dc),
            device_id_type=mesh_id,
        )

    each_around(lambda k: comp_pair(k, True).start())
    next_wave()

    put_linked(0, gain, re, im)
    part[...] = share_of(M, length)
    last = MS - 1
    take_fresh(last)
    fresh_fields(last)
    joint = Coherence()
    joint.add(range(M), PAIRS, fresh_field)
    while pending:
        next_wave()

    each_around(lambda k: comp_pair(k, False).wait_recv())
    for side, value in enumerate(gather_halo(lambda j: cpack_recv[j])):
        chalo[side] = value
    late_fields(last)
    joint.add([M], LATE_PAIRS, late_field)
    length, gain, re, im = joint.power()
    lane_line = lax.broadcasted_iota(jnp.int32, (1, cols), 1)
    part[...] = jnp.where(lane_line < cols // 2, part[...], share_of(M + 1, length))

    def reduce(count, me, device, source, buffer, sends, recvs):
        copies = []
        for step in range(1, count):
            copy = pltpu.make_async_remote_copy(
                src_ref=source,
                dst_ref=buffer.at[me],
                send_sem=sends.at[step],
                recv_sem=recvs.at[me],
                device_id=device(lax.rem(me + step, count)),
                device_id_type=mesh_id,
            )
            copy.start()
            copies.append(copy)
        buffer[me] = source[...]
        for step in range(1, count):
            other = lax.rem(me + step, count)
            pltpu.make_async_remote_copy(
                src_ref=source,
                dst_ref=buffer.at[other],
                send_sem=sends.at[step],
                recv_sem=recvs.at[other],
                device_id=device(other),
                device_id_type=mesh_id,
            ).wait_recv()
        for copy in copies:
            copy.wait_send()
        total = buffer[0]
        for other in range(1, count):
            total = total + buffer[other]
        return total

    def close_last():
        comp_re, comp_im = finish(last, M + 1, length, gain, re, im)
        comp_out[0] = comp_re
        comp_out[1] = comp_im
        put_linked(last, gain, re, im)

    def flips(position, count):
        steps = []
        size = 1
        while size < count:
            steps.append(size * (1 - 2 * lax.rem(position // size, 2)))
            size *= 2
        return steps

    def swapped(position, steps, mask_bits):
        for bit, step in enumerate(steps):
            if mask_bits >> bit & 1:
                position = position + step
        return position

    if direct:
        count = row_count * col_count
        row_steps, col_steps = flips(my_row, row_count), flips(my_col, col_count)

        def weight(code):
            return -bin(code // col_count).count("1") - code % col_count

        for code in sorted(range(1, count), key=weight):
            pltpu.make_async_remote_copy(
                src_ref=part,
                dst_ref=red_row.at[code],
                send_sem=send_r.at[0],
                recv_sem=recv_r.at[0],
                device_id=(
                    swapped(my_row, row_steps, code // col_count),
                    swapped(my_col, col_steps, code % col_count),
                ),
                device_id_type=mesh_id,
            ).start()
        close_last()
        everything = pltpu.make_async_remote_copy(
            src_ref=red_row.at[pl.ds(1, count - 1)],
            dst_ref=red_row.at[pl.ds(1, count - 1)],
            send_sem=send_r.at[0],
            recv_sem=recv_r.at[0],
            device_id=(swapped(my_row, row_steps, row_count - 1), swapped(my_col, col_steps, col_count - 1)),
            device_id_type=mesh_id,
        )
        everything.wait_recv()
        values = [part[...]] + [red_row[code] for code in range(1, count)]
        while len(values) > 1:
            values = [values[k] + values[k + 1] for k in range(0, len(values), 2)]
        total = values[0]
        strength[...] = total
        everything.wait_send()
    else:
        total = reduce(row_count, my_row, lambda d: (d, my_col), part, red_row, send_r, recv_r)
        part2 = red_col.at[col_count]
        part2[...] = total
        total = reduce(col_count, my_col, lambda d: (my_row, d), part2, red_col, send_c, recv_c)
        strength[...] = total
        close_last()

    for m in range(MS):
        each_around(lambda k, m=m: fresh_pair(m, k, True).wait_send())
    each_around(lambda k: comp_pair(k, True).wait_send())


def closing(pixels, linked_in, comp_in, total, linked, comp, strength, scalars, sems):
    copies = [
        pltpu.make_async_copy(linked_in, linked, sems.at[0]),
        pltpu.make_async_copy(comp_in, comp, sems.at[1]),
        pltpu.make_async_copy(scalars, strength, sems.at[2]),
    ]
    for copy in copies[:2]:
        copy.start()
    for m in range(MS):
        lane = lax.broadcasted_iota(jnp.int32, total.shape, 1)
        mine = lane < total.shape[1] // 2 if m == 0 else lane >= total.shape[1] // 2
        scalars[m] = jnp.sum(jnp.where(mine, total[...], 0.0)) / pixels
    copies[2].start()
    for copy in copies:
        copy.wait()


def shards(slc_stack, land_mask):
    rows, cols = land_mask.shape
    row_count, col_count = lax.axis_size("row"), lax.axis_size("col")
    f32, bf16 = jnp.float32, jnp.bfloat16
    vmem = pl.BlockSpec(memory_space=pltpu.VMEM)
    dma = pltpu.SemaphoreType.DMA
    hbm = pl.BlockSpec(memory_space=pltpu.HBM)
    devices = row_count * col_count
    direct = devices <= 64 and row_count & (row_count - 1) == 0 and col_count & (col_count - 1) == 0
    peers = devices if direct else row_count
    linked_shape = jax.ShapeDtypeStruct(slc_stack.shape, f32)
    comp_shape = jax.ShapeDtypeStruct((2, rows, cols), f32)
    linked, comp, total = pl.pallas_call(
        functools.partial(kernel, row_count, col_count, direct),
        out_shape=(linked_shape, comp_shape, jax.ShapeDtypeStruct((1, cols), f32)),
        in_specs=[hbm, hbm],
        out_specs=(vmem, vmem, vmem),
        scratch_shapes=[
            pltpu.VMEM(slc_stack.shape, f32),
            pltpu.VMEM((rows, cols), jnp.int32),
            pltpu.VMEM((MS, rows * LINE + SUB, cols), f32),
            pltpu.VMEM((MS, EDGE + SUB, cols), f32),
            pltpu.VMEM((MS, EDGE + SUB, cols), f32),
            pltpu.VMEM((MS, 2, PACK, cols), f32),
            pltpu.VMEM((MS, 6, PACK, cols), f32),
            pltpu.VMEM((MS, 2, PACK, cols), f32),
            pltpu.VMEM((2 * rows, cols), f32),
            pltpu.VMEM((2 * rows, cols), f32),
            pltpu.VMEM((2 * rows, cols), f32),
            pltpu.VMEM((2, SUB, cols), f32),
            pltpu.VMEM((6, SUB, cols), f32),
            pltpu.VMEM((2, SUB, cols), f32),
            pltpu.VMEM((2 * cols, cols), bf16),
            pltpu.VMEM((2 * cols, rows * cols), bf16),
            pltpu.VMEM((len(GROUPS), rows * 2 * SUB, 2 * cols), bf16),
            pltpu.VMEM((2, FRESH_ROWS, 2 * cols), bf16),
            pltpu.VMEM((rows, FRESH_ROWS, cols), f32),
            pltpu.VMEM((rows * FRESH_STEP, cols), f32),
            pltpu.VMEM((rows * LATE_STEP, cols), f32),
            pltpu.VMEM((SLOTS, rows, cols), f32),
            pltpu.VMEM((1, cols), f32),
            pltpu.VMEM((peers, 1, cols), f32),
            pltpu.VMEM((col_count + 1, 1, cols), f32),
            dma((2,)),
            pltpu.SemaphoreType.REGULAR((max(1, len(waves(row_count, col_count))),)),
            dma((MS, len(AROUND))),
            dma((MS, len(AROUND))),
            dma((len(AROUND),)),
            dma((len(AROUND),)),
            dma((peers,)),
            dma((peers,)),
            dma((col_count,)),
            dma((col_count,)),
        ],
        compiler_params=pltpu.CompilerParams(collective_id=0, has_side_effects=True, vmem_limit_bytes=16 << 20),
        name="linker",
    )(*(pltpu.with_memory_space_constraint(x, pltpu.HBM) for x in (slc_stack, land_mask)))
    return pl.pallas_call(
        functools.partial(closing, rows * cols * devices),
        out_shape=(linked_shape, comp_shape, jax.ShapeDtypeStruct((MS,), f32)),
        in_specs=[vmem, vmem, vmem],
        out_specs=(hbm, hbm, hbm),
        scratch_shapes=[pltpu.SMEM((MS,), f32), dma((3,))],
        compiler_params=pltpu.CompilerParams(vmem_limit_bytes=4 << 20),
        name="closing",
    )(linked, comp, total)


def solution(mesh):
    return jax.shard_map(
        shards,
        mesh=mesh,
        in_specs=(P(None, None, "row", "col"), P("row", "col")),
        out_specs=(P(None, None, "row", "col"), P(None, "row", "col"), P()),
        check_vma=False,
    )
```

```python
import functools

import jax
import jax.numpy as jnp
from jax import lax
from jax.experimental import pallas as pl
from jax.experimental.pallas import tpu as pltpu
from jax.sharding import PartitionSpec as P

M = 10
MS = 2
WIN = 11
ITERS = 4
REACH = WIN // 2
SUB = 8

covariance_floor = 8.0

AROUND = ((-1, 0), (1, 0), (-1, -1), (0, -1), (1, -1), (-1, 1), (0, 1), (1, 1))
LINE = 2 * M
EDGE = -(-REACH * LINE // SUB) * SUB
SKIP = EDGE - REACH * LINE
PACK = -(-LINE // SUB) * SUB


def pair_groups():
    groups = [[(s, (s + lag) % SUB) for s in range(SUB)] for lag in range(SUB // 2)]
    half = SUB // 2
    groups.append([(s, s + half) for s in range(half)] + [(M - 2, M - 1), (M - 2, M - 2), (M - 1, M - 1)])
    groups.append([(s, M - 2) for s in range(SUB)])
    groups.append([(s, M - 1) for s in range(SUB)])
    return groups


def field_rows(groups):
    table = {}
    for unit, group in enumerate(groups):
        for lane, (i, j) in enumerate(group):
            for part in range(1 if i == j else 2):
                table[(i, j, part)] = unit * 2 * SUB + part * SUB + lane
    return table


GROUPS = pair_groups()
LATE = [[(s, M) for s in range(SUB)], [(M, M)] * (2 * SUB - M) + [(s, M) for s in range(SUB, M)]]
FIELDS = field_rows(GROUPS)
LATE_FIELDS = field_rows(LATE)
PAIRS = [(i, j) for i, j, part in FIELDS if part == 1]
LATE_PAIRS = [(i, j) for i, j, part in LATE_FIELDS if part == 1]
FRESH_ROWS = len(GROUPS) * 2 * SUB
LATE_ROWS = len(LATE) * 2 * SUB
FRESH_STEP = FRESH_ROWS + 4
LATE_STEP = LATE_ROWS + 4
SLOTS = 3 * (len(PAIRS) + len(LATE_PAIRS)) + M + 1


def own_range(r, rows):
    return max(r, REACH), min(r + WIN, REACH + rows)


def own_sums(lines, rows):
    core = lines[rows - 1 - REACH]
    for e in range(rows, WIN):
        core = core + lines[e - REACH]
    starts = {rows - 1: core}
    for e in range(rows - 2, REACH - 1, -1):
        starts[e] = starts[e + 1] + lines[e - REACH]
    tails = {WIN: None}
    for e in range(WIN, REACH + rows):
        tails[e + 1] = lines[e - REACH] if tails[e] is None else tails[e] + lines[e - REACH]
    sums = {}
    for r in range(rows):
        start, stop = own_range(r, rows)
        if (start, stop) not in sums:
            tail = tails[stop]
            sums[(start, stop)] = starts[start] if tail is None else starts[start] + tail
    return sums


def window_sums(above, below, partial, rows):
    lead = {REACH: None}
    for e in range(REACH - 1, -1, -1):
        lead[e] = above[e] if lead[e + 1] is None else lead[e + 1] + above[e]
    trail = {0: None}
    for e in range(REACH):
        trail[e + 1] = below[e] if trail[e] is None else trail[e] + below[e]
    sums = []
    for r in range(rows):
        total = partial(r)
        for extra in (lead[min(r, REACH)], trail[max(0, r + WIN - REACH - rows)]):
            if extra is not None:
                total = total + extra
        sums.append(total)
    return sums


def split(value):
    high = value.astype(jnp.bfloat16)
    low = (value - high.astype(jnp.float32)).astype(jnp.bfloat16)
    return high, low


def waves(row_count, col_count):
    offsets = []
    known = 1
    while known < max(row_count, col_count) - 1:
        offsets.append(known)
        known *= 2
    return offsets


def kernel(
    row_count,
    col_count,
    direct,
    slc_hbm,
    land_hbm,
    linked,
    comp_out,
    strength,
    slc,
    land,
    own,
    up,
    dn,
    pack_send,
    pack_recv,
    halo,
    comp_send,
    comp_up,
    comp_dn,
    cpack_send,
    cpack_recv,
    chalo,
    w_main,
    w_halo,
    pbuf,
    ybuf,
    hbuf,
    ebuf,
    zbuf,
    zcbuf,
    coh,
    part,
    red_row,
    red_col,
    load_sem,
    ready,
    send_a,
    recv_a,
    send_b,
    recv_b,
    send_r,
    recv_r,
):
    rows, cols = land.shape
    my_row = lax.axis_index("row")
    my_col = lax.axis_index("col")
    strip = rows * REACH
    mesh_id = pl.DeviceIdType.MESH
    loads = [
        pltpu.make_async_copy(land_hbm, land, load_sem.at[MS]),
    ] + [
        pltpu.make_async_copy(slc_hbm.at[pl.ds(m * M, M)], slc.at[pl.ds(m * M, M)], load_sem.at[m]) for m in range(MS)
    ]
    for load in loads:
        load.start()

    def existing(dr, dc, far=1):
        ok = None
        for pos, step, count in ((my_row, dr, row_count), (my_col, dc, col_count)):
            if step:
                here = (pos >= far) if step < 0 else (pos < count - far)
                ok = here if ok is None else jnp.logical_and(ok, here)
        return ok

    exists = [existing(dr, dc) for dr, dc in AROUND]

    def greet(semaphore, far):
        expected = jnp.int32(0)
        for k, (dr, dc) in enumerate(AROUND):
            if (dr and far >= row_count) or (dc and far >= col_count):
                continue
            there = existing(dr, dc, far)

            @pl.when(there)
            def _(dr=dr, dc=dc):
                pl.semaphore_signal(
                    semaphore,
                    inc=1,
                    device_id=(my_row + dr * far, my_col + dc * far),
                    device_id_type=mesh_id,
                )

            expected = expected + there.astype(jnp.int32)
        return expected

    barrier = pltpu.get_barrier_semaphore()
    expected = greet(barrier, 1)
    offsets = waves(row_count, col_count)
    pending = []

    def next_wave():
        if pending:
            index, count = pending.pop()
            pl.semaphore_wait(ready.at[index], count)
            index += 1
        else:
            index = 0
        if index < len(offsets):
            pending.append((index, greet(ready.at[index], offsets[index])))

    for k, (dr, dc) in enumerate(AROUND):

        @pl.when(jnp.logical_not(exists[k]))
        def _(k=k, dc=dc, dr=dr):
            if dc == 0:
                target, small = (up, comp_up) if dr < 0 else (dn, comp_dn)
                for m in range(MS):
                    target[m] = jnp.zeros(target.shape[1:], jnp.float32)
                small[...] = jnp.zeros_like(small)
            else:
                for m in range(MS):
                    pack_recv[m, k - 2] = jnp.zeros(pack_recv.shape[2:], jnp.float32)
                cpack_recv[k - 2] = jnp.zeros(cpack_recv.shape[1:], jnp.float32)

    lane = lax.broadcasted_iota(jnp.int32, (rows, cols), 1)
    sub = lax.broadcasted_iota(jnp.int32, (rows, cols), 0)

    for load in loads[:2]:
        load.wait()
    mask = land[...].astype(jnp.float32)

    def place(m):
        for i in range(M):
            for c in range(2):
                own[m, pl.ds(c * M + i, rows, stride=LINE), :] = slc[m * M + i, c] * mask
        own[m, rows * LINE :, :] = jnp.zeros((own.shape[1] - rows * LINE, cols), jnp.float32)

    def spread(line, shift):
        total = pltpu.roll(line, cols - shift, 1) if shift else line
        return (
            total
            + pltpu.roll(line, (strip - shift) % cols, 1)
            + pltpu.roll(line, (2 * strip - shift) % cols, 1)
        )

    def pack(m):
        for at in range(0, PACK, SUB):
            low = high = jnp.zeros((SUB, cols), jnp.float32)
            for r in range(rows):
                turned = pltpu.roll(own[m, r * LINE + at : r * LINE + at + SUB, :], REACH * (r + 1), 1)
                high = jnp.where((lane >= r * REACH) & (lane < (r + 1) * REACH), turned, high)
                low = jnp.where((lane >= (r + 1) * REACH) & (lane < (r + 2) * REACH), turned, low)
            pack_send[m, 0, at : at + SUB, :] = spread(low, REACH)
            pack_send[m, 1, at : at + SUB, :] = spread(high, 0)

    def mirror(k):
        dr, dc = AROUND[k]
        return AROUND.index((-dr, -dc))

    def fresh_pair(m, k, sending):
        dr, dc = AROUND[k]
        back = mirror(k)
        slot = back if sending else k
        if dc == 0:
            source = own.at[m, pl.ds(0 if dr < 0 else rows * LINE - EDGE, EDGE)]
            target = (up if AROUND[slot][0] < 0 else dn).at[m, pl.ds(0, EDGE)]
        else:
            source = pack_send.at[m, 0 if dc < 0 else 1]
            target = pack_recv.at[m, slot - 2]
        return pltpu.make_async_remote_copy(
            src_ref=source,
            dst_ref=target,
            send_sem=send_a.at[k],
            recv_sem=recv_a.at[m, slot],
            device_id=(my_row + dr, my_col + dc),
            device_id_type=mesh_id,
        )

    def each_around(action, which=range(len(AROUND))):
        for k in which:

            @pl.when(exists[k])
            def _(k=k):
                action(k)

    beside, strips = range(2), range(2, len(AROUND))
    place(0)
    pl.semaphore_wait(barrier, expected)
    each_around(lambda k: fresh_pair(0, k, True).start(), beside)
    pack(0)
    each_around(lambda k: fresh_pair(0, k, True).start(), strips)
    next_wave()
    for m in range(1, MS):
        loads[1 + m].wait()
        place(m)
        pack(m)
        each_around(lambda k, m=m: fresh_pair(m, k, True).start())

    k_at = lax.broadcasted_iota(jnp.int32, (cols, cols), 0)
    n_at = lax.broadcasted_iota(jnp.int32, (cols, cols), 1)
    near = jnp.where((k_at - n_at <= REACH) & (n_at - k_at <= REACH), 1.0, 0.0).astype(jnp.bfloat16)
    w_main[0:cols, :] = near
    w_main[cols:, :] = near
    line_of = k_at // REACH
    inner = k_at - line_of * REACH
    for side in range(2):
        touches = (n_at <= inner) if side == 0 else (n_at >= inner + cols - REACH)
        line = jnp.where(touches, line_of, -1)
        for r in range(rows):
            first = rows - REACH + r
            w_halo[side * cols : (side + 1) * cols, r * cols : (r + 1) * cols] = jnp.where(
                (line >= first) & (line < first + WIN), 1.0, 0.0
            ).astype(jnp.bfloat16)

    lines_total = WIN + rows - 1

    def gather_halo(parts):
        sides = []
        for side in range(2):
            a, b, c = (parts(side * 3 + j) for j in range(3))
            which = lax.broadcasted_iota(jnp.int32, a.shape, 1)
            sides.append(jnp.where(which < strip, a, jnp.where(which < 2 * strip, b, c)))
        return sides

    def line_tile(m, e, c, first):
        if e < REACH:
            buffer, at = up, SKIP + e * LINE
        elif e < REACH + rows:
            buffer, at = own, (e - REACH) * LINE
        else:
            buffer, at = dn, (e - REACH - rows) * LINE
        at += c * M + first
        return buffer[m, at : at + SUB, :]

    def halo_tile(m, side, c, first):
        at = c * M + first
        return halo[m, side, at : at + SUB, :]

    def real_part(a, b, x, y):
        return a * x + b * y

    def imag_part(a, b, x, y):
        return b * x - a * y

    def operands(tile, unit):
        lead = [tile(c, 0) for c in range(2)]
        if unit == 0:
            return lead, lead
        if unit < SUB // 2:
            return lead, [pltpu.roll(v, SUB - unit, 0) for v in lead]
        if unit == SUB // 2:
            left, right = [], []
            for c in range(2):
                mid, late = tile(c, SUB // 2), tile(c, SUB - M + 5)
                left.append(jnp.where(sub < 4, lead[c], jnp.where(sub == 4, mid, late)))
                right.append(jnp.where(sub < 4, mid, jnp.where(sub == 4, tile(c, 5), late)))
            return left, right
        return lead, None

    def products(tile, row_tile, unit):
        (a, b), other = operands(tile, unit)
        if unit == 0:
            return a * a + b * b, None
        if other is None:
            image = M - 3 + unit - SUB // 2
            x, y = (jnp.broadcast_to(row_tile(c, image), (SUB, cols)) for c in range(2))
        else:
            x, y = other
        return real_part(a, b, x, y), imag_part(a, b, x, y)

    def tile_of(m, e):
        if e < lines_total:
            return functools.partial(line_tile, m, e)
        return functools.partial(halo_tile, m, e - lines_total)

    def row_of(m, e):
        tile = tile_of(m, e)
        return lambda c, image: tile(c, image)[0:1]

    def emit_side(unit, side, value):
        high, low = split(value)
        at = slice(unit * 2 * SUB, (unit + 1) * 2 * SUB)
        hbuf[0, at, side * cols : (side + 1) * cols] = high
        hbuf[1, at, side * cols : (side + 1) * cols] = low

    def edges(count):
        for r in range(0, rows, 2):
            band = w_halo[:, r * cols : (r + 2) * cols]
            value = jnp.dot(hbuf[0, 0:count], band, preferred_element_type=jnp.float32) + jnp.dot(
                hbuf[1, 0:count], band, preferred_element_type=jnp.float32
            )
            ebuf[r, 0:count] = value[:, 0:cols]
            ebuf[r + 1, 0:count] = value[:, cols:]

    partials = {}
    for r in range(rows):
        partials.setdefault(own_range(r, rows), len(partials))

    def keep_own(unit, lines):
        for key, value in own_sums(lines, rows).items():
            at = (unit * len(partials) + partials[key]) * 2 * SUB
            pbuf[at : at + 2 * SUB, :] = value

    def emit_lines(unit, lines, target, step):
        def partial(r):
            at = (unit * len(partials) + partials[own_range(r, rows)]) * 2 * SUB
            return pbuf[at : at + 2 * SUB, :]

        for r, total in enumerate(window_sums(lines[:REACH], lines[REACH:], partial, rows)):
            high, low = split(total)
            ybuf[unit, r * 2 * SUB : (r + 1) * 2 * SUB, 0:cols] = high
            ybuf[unit, r * 2 * SUB : (r + 1) * 2 * SUB, cols:] = low
        main = jnp.dot(ybuf[unit], w_main[...], preferred_element_type=jnp.float32)
        for r in range(rows):
            at = r * step + unit * 2 * SUB
            target[at : at + 2 * SUB, :] = (
                main[r * 2 * SUB : (r + 1) * 2 * SUB, :] + ebuf[r, unit * 2 * SUB : (unit + 1) * 2 * SUB]
            )

    def both_halves(pair):
        first, second = pair
        return jnp.concatenate([first, jnp.zeros_like(first) if second is None else second], 0)

    own_lines = range(REACH, REACH + rows)
    far_lines = [*range(REACH), *range(REACH + rows, lines_total)]

    def fresh_values(m, e, unit):
        return both_halves(products(tile_of(m, e), row_of(m, e), unit))

    def fresh_own(m):
        for unit in range(len(GROUPS)):
            keep_own(unit, [fresh_values(m, e, unit) for e in own_lines])

    def fresh_sides(m):
        for side in range(2):
            for unit in range(len(GROUPS)):
                emit_side(unit, side, fresh_values(m, lines_total + side, unit))
        edges(FRESH_ROWS)

    def fresh_far(m):
        for unit in range(len(GROUPS)):
            emit_lines(unit, [fresh_values(m, e, unit) for e in far_lines], zbuf, FRESH_STEP)

    def comp_row(e, c):
        if e < REACH:
            at = c * rows + rows - REACH + e
            return comp_up[at : at + 1, :]
        if e < REACH + rows:
            at = c * rows + e - REACH
            return comp_send[at : at + 1, :]
        if e < lines_total:
            at = c * rows + e - REACH - rows
            return comp_dn[at : at + 1, :]
        return chalo[e - lines_total, c : c + 1, :]

    def late_products(m, e, unit):
        tile = tile_of(m, e)
        x, y = (jnp.broadcast_to(comp_row(e, c), (SUB, cols)) for c in range(2))
        if unit == 0:
            a, b = tile(0, 0), tile(1, 0)
        else:
            a, b = (jnp.where(sub < 2 * SUB - M, v, tile(c, M - SUB)) for c, v in enumerate((x, y)))
        return jnp.concatenate([real_part(a, b, x, y), imag_part(a, b, x, y)], 0)

    def late_fields(m):
        for side in range(2):
            for unit in range(len(LATE)):
                emit_side(unit, side, late_products(m, lines_total + side, unit))
        edges(LATE_ROWS)
        for unit in range(len(LATE)):
            emit_lines(unit, [late_products(m, e, unit) for e in far_lines], zcbuf, LATE_STEP)

    def late_own(m):
        for unit in range(len(LATE)):
            keep_own(unit, [late_products(m, e, unit) for e in own_lines])

    def fresh_field(i, j, p):
        return zbuf[pl.ds(FIELDS[(i, j, p)], rows, stride=FRESH_STEP), :]

    def late_field(i, j, p):
        return zcbuf[pl.ds(LATE_FIELDS[(i, j, p)], rows, stride=LATE_STEP), :]

    class Coherence:
        def __init__(self):
            self.scales = {}
            self.slot = {}
            self.re = {}
            self.im = {}
            self.used = 0

        def keep(self, key, value):
            coh[self.used] = value
            self.slot[key] = self.used
            self.used += 1

        def get(self, key):
            return coh[self.slot[key]]

        def tally(self, sums, i, value, minus=False):
            if i in sums:
                sums[i] = sums[i] - value if minus else sums[i] + value
            else:
                sums[i] = -value if minus else value

        def add(self, images, pairs, field):
            for i in images:
                value = field(i, i, 0)
                scale = lax.rsqrt(jnp.maximum(value, covariance_floor))
                self.scales[i] = scale
                value = value * (scale * scale)
                self.keep((i, i), value)
                self.tally(self.re, i, value)
            for i, j in pairs:
                s = self.scales[i] * self.scales[j]
                c = field(i, j, 0) * s
                d = field(i, j, 1) * s
                self.keep((i, j, 0), c)
                self.keep((i, j, 1), c + d)
                self.keep((i, j, 2), c - d)
                self.tally(self.re, i, c)
                self.tally(self.re, j, c)
                self.tally(self.im, i, d)
                self.tally(self.im, j, d, True)

        def power(self):
            images = sorted(self.re)
            re = [self.re[i] for i in images]
            im = [self.im[i] for i in images]
            gain = None
            for step in range(ITERS):
                if step:
                    both = [x + y for x, y in zip(re, im)]
                    new_re, new_im = [], []
                    for i in images:
                        shared = first = second = None
                        for j in images:
                            if j == i:
                                continue
                            key = (i, j) if (i, j, 0) in self.slot else (j, i)
                            turn = key != (i, j)
                            c = self.get(key + (0,)) * both[j]
                            e = self.get(key + (2 if turn else 1,)) * im[j]
                            f = self.get(key + (1 if turn else 2,)) * re[j]
                            shared = c if shared is None else shared + c
                            first = e if first is None else first + e
                            second = f if second is None else second + f
                        c = self.get((i, i))
                        new_re.append((shared - first) + c * re[i])
                        new_im.append((shared - second) + c * im[i])
                    re, im = new_re, new_im
                squares = [x * x + y * y for x, y in zip(re, im)]
                while len(squares) > 1:
                    squares = [sum(squares[k + 1 : k + 2], squares[k]) for k in range(0, len(squares), 2)]
                length = jnp.sqrt(squares[0])
                if gain is not None:
                    length = length * gain
                inverse = 1.0 / jnp.maximum(length, 1.0)
                gain = inverse if gain is None else gain * inverse
            return length, gain, re, im

    def finish(m, number, length, gain, re, im):
        comp_re = comp_im = None
        for i in range(M):
            a = own[m, pl.ds(i, rows, stride=LINE), :]
            b = own[m, pl.ds(M + i, rows, stride=LINE), :]
            x = re[i] * a + im[i] * b
            y = re[i] * b - im[i] * a
            comp_re = x if comp_re is None else comp_re + x
            comp_im = y if comp_im is None else comp_im + y
        return comp_re * gain, comp_im * gain

    def put_linked(m, gain, re, im):
        factor = gain * mask
        for i in range(M):
            linked[m * M + i, 0] = re[i] * factor
            linked[m * M + i, 1] = im[i] * factor

    def share_of(number, length):
        return jnp.sum(mask * length, axis=0, keepdims=True) * (1.0 / number)

    def take_strips(m):
        each_around(lambda k: fresh_pair(m, k, False).wait_recv(), strips)
        for side, value in enumerate(gather_halo(lambda j: pack_recv[m, j])):
            halo[m, side] = value

    def take_beside(m):
        each_around(lambda k: fresh_pair(m, k, False).wait_recv(), beside)

    fresh_own(0)
    take_strips(0)
    fresh_sides(0)
    next_wave()
    take_beside(0)
    fresh_far(0)
    early = Coherence()
    early.add(range(M), PAIRS, fresh_field)
    length, gain, re, im = early.power()
    comp_re, comp_im = finish(0, M, length, gain, re, im)
    comp_send[0:rows, :] = comp_re
    comp_send[rows:, :] = comp_im

    def comp_pair(k, sending):
        dr, dc = AROUND[k]
        slot = mirror(k) if sending else k
        if dc == 0:
            source = comp_send
            target = comp_up if AROUND[slot][0] < 0 else comp_dn
        else:
            source = cpack_send.at[0 if dc < 0 else 1]
            target = cpack_recv.at[slot - 2]
        return pltpu.make_async_remote_copy(
            src_ref=source,
            dst_ref=target,
            send_sem=send_b.at[k],
            recv_sem=recv_b.at[slot],
            device_id=(my_row + dr, my_col + dc),
            device_id_type=mesh_id,
        )

    each_around(lambda k: comp_pair(k, True).start(), beside)
    cpack_send[...] = jnp.zeros_like(cpack_send)
    for c, value in enumerate((comp_re, comp_im)):
        for side in range(2):
            total = jnp.zeros((rows, cols), jnp.float32)
            for copy in range(3):
                turned = pltpu.roll(value, REACH * side + strip * copy, 1, stride=REACH, stride_axis=0)
                first = strip * copy + sub * REACH
                total = jnp.where((lane >= first) & (lane < first + REACH), turned, total)
            cpack_send[side, c : c + 1, :] = jnp.sum(total, axis=0, keepdims=True)

    each_around(lambda k: comp_pair(k, True).start(), (2, 4, 5, 7, 3, 6))

    put_linked(0, gain, re, im)
    part[0:1] = share_of(M, length)
    last = MS - 1
    fresh_own(last)
    take_strips(last)
    fresh_sides(last)
    take_beside(last)
    fresh_far(last)
    late_own(last)
    joint = Coherence()
    joint.add(range(M), PAIRS, fresh_field)
    while len(pending) and pending[0][0] < len(offsets) - 1:
        next_wave()

    each_around(lambda k: comp_pair(k, False).wait_recv())
    for side, value in enumerate(gather_halo(lambda j: cpack_recv[j])):
        chalo[side] = value
    late_fields(last)
    joint.add([M], LATE_PAIRS, late_field)
    length, gain, re, im = joint.power()
    part[last : last + 1] = share_of(M + 1, length)
    while pending:
        next_wave()

    def reduce(count, me, device, source, buffer, sends, recvs):
        copies = []
        for step in range(1, count):
            copy = pltpu.make_async_remote_copy(
                src_ref=source,
                dst_ref=buffer.at[me],
                send_sem=sends.at[step],
                recv_sem=recvs.at[me],
                device_id=device(lax.rem(me + step, count)),
                device_id_type=mesh_id,
            )
            copy.start()
            copies.append(copy)
        buffer[me] = source[...]
        for step in range(1, count):
            other = lax.rem(me + step, count)
            pltpu.make_async_remote_copy(
                src_ref=source,
                dst_ref=buffer.at[other],
                send_sem=sends.at[step],
                recv_sem=recvs.at[other],
                device_id=device(other),
                device_id_type=mesh_id,
            ).wait_recv()
        for copy in copies:
            copy.wait_send()
        total = buffer[0]
        for other in range(1, count):
            total = total + buffer[other]
        return total

    def close_last():
        comp_re, comp_im = finish(last, M + 1, length, gain, re, im)
        comp_out[0] = comp_re
        comp_out[1] = comp_im
        put_linked(last, gain, re, im)

    def sent(k):
        dr, dc = AROUND[k]
        if dc == 0:
            source, target = own.at[:, pl.ds(0, EDGE)], up.at[:, pl.ds(0, EDGE)]
        else:
            source, target = pack_send.at[:, 0], pack_recv.at[:, 0]
        return pltpu.make_async_remote_copy(
            src_ref=source,
            dst_ref=target,
            send_sem=send_a.at[k],
            recv_sem=recv_a.at[0, k],
            device_id=(my_row + dr, my_col + dc),
            device_id_type=mesh_id,
        )

    def finish_sends():
        each_around(lambda k: sent(k).wait_send())
        each_around(lambda k: comp_pair(k, True).wait_send())

    def flips(position, count):
        steps = []
        size = 1
        while size < count:
            steps.append(size * (1 - 2 * lax.rem(position // size, 2)))
            size *= 2
        return steps

    def swapped(position, steps, mask_bits):
        for bit, step in enumerate(steps):
            if mask_bits >> bit & 1:
                position = position + step
        return position

    if direct:
        count = row_count * col_count
        row_steps, col_steps = flips(my_row, row_count), flips(my_col, col_count)

        def weight(code):
            return -bin(code // col_count).count("1") - code % col_count

        for code in sorted(range(1, count), key=weight):
            pltpu.make_async_remote_copy(
                src_ref=part,
                dst_ref=red_row.at[code],
                send_sem=send_r.at[0],
                recv_sem=recv_r.at[0],
                device_id=(
                    swapped(my_row, row_steps, code // col_count),
                    swapped(my_col, col_steps, code % col_count),
                ),
                device_id_type=mesh_id,
            ).start()
        close_last()
        finish_sends()
        everything = pltpu.make_async_remote_copy(
            src_ref=red_row.at[pl.ds(1, count - 1)],
            dst_ref=red_row.at[pl.ds(1, count - 1)],
            send_sem=send_r.at[0],
            recv_sem=recv_r.at[0],
            device_id=(swapped(my_row, row_steps, row_count - 1), swapped(my_col, col_steps, col_count - 1)),
            device_id_type=mesh_id,
        )
        everything.wait_recv()
        values = [part[...]] + [red_row[code] for code in range(1, count)]
        while len(values) > 1:
            values = [values[k] + values[k + 1] for k in range(0, len(values), 2)]
        total = values[0]
        strength[...] = total
        everything.wait_send()
    else:
        total = reduce(row_count, my_row, lambda d: (d, my_col), part, red_row, send_r, recv_r)
        part2 = red_col.at[col_count]
        part2[...] = total
        total = reduce(col_count, my_col, lambda d: (my_row, d), part2, red_col, send_r.at[pl.ds(row_count, col_count)], recv_r.at[pl.ds(row_count, col_count)])
        strength[...] = total
        close_last()
        finish_sends()


def closing(pixels, linked_in, comp_in, total, linked, comp, strength, scalars, sems):
    copies = [
        pltpu.make_async_copy(linked_in, linked, sems.at[0]),
        pltpu.make_async_copy(comp_in, comp, sems.at[1]),
        pltpu.make_async_copy(scalars, strength, sems.at[2]),
    ]
    for copy in copies[:2]:
        copy.start()
    for m in range(MS):
        scalars[m] = jnp.sum(total[m : m + 1]) / pixels
    copies[2].start()
    for copy in copies:
        copy.wait()


def shards(slc_stack, land_mask):
    rows, cols = land_mask.shape
    row_count, col_count = lax.axis_size("row"), lax.axis_size("col")
    f32, bf16 = jnp.float32, jnp.bfloat16
    vmem = pl.BlockSpec(memory_space=pltpu.VMEM)
    dma = pltpu.SemaphoreType.DMA
    hbm = pl.BlockSpec(memory_space=pltpu.HBM)
    devices = row_count * col_count
    direct = devices <= 64 and row_count & (row_count - 1) == 0 and col_count & (col_count - 1) == 0
    peers = devices if direct else row_count
    linked_shape = jax.ShapeDtypeStruct(slc_stack.shape, f32)
    comp_shape = jax.ShapeDtypeStruct((2, rows, cols), f32)
    linked, comp, total = pl.pallas_call(
        functools.partial(kernel, row_count, col_count, direct),
        out_shape=(linked_shape, comp_shape, jax.ShapeDtypeStruct((MS, cols), f32)),
        in_specs=[hbm, hbm],
        out_specs=(vmem, vmem, vmem),
        scratch_shapes=[
            pltpu.VMEM(slc_stack.shape, f32),
            pltpu.VMEM((rows, cols), jnp.int32),
            pltpu.VMEM((MS, rows * LINE + SUB, cols), f32),
            pltpu.VMEM((MS, EDGE + SUB, cols), f32),
            pltpu.VMEM((MS, EDGE + SUB, cols), f32),
            pltpu.VMEM((MS, 2, PACK, cols), f32),
            pltpu.VMEM((MS, 6, PACK, cols), f32),
            pltpu.VMEM((MS, 2, PACK, cols), f32),
            pltpu.VMEM((2 * rows, cols), f32),
            pltpu.VMEM((2 * rows, cols), f32),
            pltpu.VMEM((2 * rows, cols), f32),
            pltpu.VMEM((2, SUB, cols), f32),
            pltpu.VMEM((6, SUB, cols), f32),
            pltpu.VMEM((2, SUB, cols), f32),
            pltpu.VMEM((2 * cols, cols), bf16),
            pltpu.VMEM((2 * cols, rows * cols), bf16),
            pltpu.VMEM((len(GROUPS) * rows * 2 * SUB, cols), f32),
            pltpu.VMEM((len(GROUPS), rows * 2 * SUB, 2 * cols), bf16),
            pltpu.VMEM((2, FRESH_ROWS, 2 * cols), bf16),
            pltpu.VMEM((rows, FRESH_ROWS, cols), f32),
            pltpu.VMEM((rows * FRESH_STEP, cols), f32),
            pltpu.VMEM((rows * LATE_STEP, cols), f32),
            pltpu.VMEM((SLOTS, rows, cols), f32),
            pltpu.VMEM((MS, cols), f32),
            pltpu.VMEM((peers, MS, cols), f32),
            pltpu.VMEM((col_count + 1, MS, cols), f32),
            dma((MS + 1,)),
            pltpu.SemaphoreType.REGULAR((max(1, len(waves(row_count, col_count))),)),
            dma((len(AROUND),)),
            dma((MS, len(AROUND))),
            dma((len(AROUND),)),
            dma((len(AROUND),)),
            dma((1 if direct else row_count + col_count,)),
            dma((1 if direct else row_count + col_count,)),
        ],
        compiler_params=pltpu.CompilerParams(collective_id=0, has_side_effects=True, vmem_limit_bytes=16 << 20),
        name="linker",
    )(*(pltpu.with_memory_space_constraint(x, pltpu.HBM) for x in (slc_stack, land_mask)))
    return pl.pallas_call(
        functools.partial(closing, rows * cols * devices),
        out_shape=(linked_shape, comp_shape, jax.ShapeDtypeStruct((MS,), f32)),
        in_specs=[vmem, vmem, vmem],
        out_specs=(hbm, hbm, hbm),
        scratch_shapes=[pltpu.SMEM((MS,), f32), dma((3,))],
        compiler_params=pltpu.CompilerParams(vmem_limit_bytes=4 << 20),
        name="closing",
    )(linked, comp, total)


def solution(mesh):
    return jax.shard_map(
        shards,
        mesh=mesh,
        in_specs=(P(None, None, "row", "col"), P("row", "col")),
        out_specs=(P(None, None, "row", "col"), P(None, "row", "col"), P()),
        check_vma=False,
    )
```

```python
import functools

import jax
import jax.numpy as jnp
from jax import lax
from jax.experimental import pallas as pl
from jax.experimental.pallas import tpu as pltpu
from jax.sharding import PartitionSpec as P

M = 10
MS = 2
WIN = 11
ITERS = 4
REACH = WIN // 2
SUB = 8

covariance_floor = 8.0

AROUND = ((-1, 0), (1, 0), (-1, -1), (0, -1), (1, -1), (-1, 1), (0, 1), (1, 1))
LINE = 2 * M
EDGE = -(-REACH * LINE // SUB) * SUB
SKIP = EDGE - REACH * LINE
PACK = -(-LINE // SUB) * SUB


def pair_groups():
    groups = [[(s, (s + lag) % SUB) for s in range(SUB)] for lag in range(SUB // 2)]
    half = SUB // 2
    groups.append([(s, s + half) for s in range(half)] + [(M - 2, M - 1), (M - 2, M - 2), (M - 1, M - 1)])
    groups.append([(s, M - 2) for s in range(SUB)])
    groups.append([(s, M - 1) for s in range(SUB)])
    return groups


def field_rows(groups):
    table = {}
    for unit, group in enumerate(groups):
        for lane, (i, j) in enumerate(group):
            for part in range(1 if i == j else 2):
                table[(i, j, part)] = unit * 2 * SUB + part * SUB + lane
    return table


GROUPS = pair_groups()
LATE = [[(s, M) for s in range(SUB)], [(M, M)] * (2 * SUB - M) + [(s, M) for s in range(SUB, M)]]
FIELDS = field_rows(GROUPS)
LATE_FIELDS = field_rows(LATE)
PAIRS = [(i, j) for i, j, part in FIELDS if part == 1]
LATE_PAIRS = [(i, j) for i, j, part in LATE_FIELDS if part == 1]
FRESH_ROWS = len(GROUPS) * 2 * SUB
LATE_ROWS = len(LATE) * 2 * SUB
FRESH_STEP = FRESH_ROWS + 4
LATE_STEP = LATE_ROWS + 4
SLOTS = 3 * (len(PAIRS) + len(LATE_PAIRS)) + M + 1


def own_range(r, rows):
    return max(r, REACH), min(r + WIN, REACH + rows)


def own_sums(lines, rows):
    core = lines[rows - 1 - REACH]
    for e in range(rows, WIN):
        core = core + lines[e - REACH]
    starts = {rows - 1: core}
    for e in range(rows - 2, REACH - 1, -1):
        starts[e] = starts[e + 1] + lines[e - REACH]
    tails = {WIN: None}
    for e in range(WIN, REACH + rows):
        tails[e + 1] = lines[e - REACH] if tails[e] is None else tails[e] + lines[e - REACH]
    sums = {}
    for r in range(rows):
        start, stop = own_range(r, rows)
        if (start, stop) not in sums:
            tail = tails[stop]
            sums[(start, stop)] = starts[start] if tail is None else starts[start] + tail
    return sums


def window_sums(above, below, partial, rows):
    lead = {REACH: None}
    for e in range(REACH - 1, -1, -1):
        lead[e] = above[e] if lead[e + 1] is None else lead[e + 1] + above[e]
    trail = {0: None}
    for e in range(REACH):
        trail[e + 1] = below[e] if trail[e] is None else trail[e] + below[e]
    sums = []
    for r in range(rows):
        total = partial(r)
        for extra in (lead[min(r, REACH)], trail[max(0, r + WIN - REACH - rows)]):
            if extra is not None:
                total = total + extra
        sums.append(total)
    return sums


def split(value):
    high = value.astype(jnp.bfloat16)
    low = (value - high.astype(jnp.float32)).astype(jnp.bfloat16)
    return high, low


def waves(row_count, col_count):
    offsets = []
    known = 1
    while known < max(row_count, col_count) - 1:
        offsets.append(known)
        known *= 2
    return offsets


def kernel(
    row_count,
    col_count,
    direct,
    slc_hbm,
    land_hbm,
    linked,
    comp_out,
    strength,
    slc,
    land,
    own,
    up,
    dn,
    pack_send,
    pack_recv,
    halo,
    comp_send,
    comp_up,
    comp_dn,
    cpack_send,
    cpack_recv,
    chalo,
    w_main,
    w_halo,
    pbuf,
    ybuf,
    hbuf,
    ebuf,
    zbuf,
    zcbuf,
    coh,
    part,
    red_row,
    red_col,
    load_sem,
    ready,
    send_a,
    recv_a,
    send_b,
    recv_b,
    send_r,
    recv_r,
):
    rows, cols = land.shape
    my_row = lax.axis_index("row")
    my_col = lax.axis_index("col")
    strip = rows * REACH
    mesh_id = pl.DeviceIdType.MESH
    loads = [
        pltpu.make_async_copy(land_hbm, land, load_sem.at[MS]),
    ] + [
        pltpu.make_async_copy(slc_hbm.at[pl.ds(m * M, M)], slc.at[pl.ds(m * M, M)], load_sem.at[m]) for m in range(MS)
    ]
    for load in loads:
        load.start()

    def existing(dr, dc, far=1):
        ok = None
        for pos, step, count in ((my_row, dr, row_count), (my_col, dc, col_count)):
            if step:
                here = (pos >= far) if step < 0 else (pos < count - far)
                ok = here if ok is None else jnp.logical_and(ok, here)
        return ok

    exists = [existing(dr, dc) for dr, dc in AROUND]

    def greet(semaphore, far):
        expected = jnp.int32(0)
        for k, (dr, dc) in enumerate(AROUND):
            if (dr and far >= row_count) or (dc and far >= col_count):
                continue
            there = existing(dr, dc, far)

            @pl.when(there)
            def _(dr=dr, dc=dc):
                pl.semaphore_signal(
                    semaphore,
                    inc=1,
                    device_id=(my_row + dr * far, my_col + dc * far),
                    device_id_type=mesh_id,
                )

            expected = expected + there.astype(jnp.int32)
        return expected

    barrier = pltpu.get_barrier_semaphore()
    expected = greet(barrier, 1)
    offsets = waves(row_count, col_count)
    pending = []

    def next_wave():
        if pending:
            index, count = pending.pop()
            pl.semaphore_wait(ready.at[index], count)
            index += 1
        else:
            index = 0
        if index < len(offsets):
            pending.append((index, greet(ready.at[index], offsets[index])))

    for k, (dr, dc) in enumerate(AROUND):

        @pl.when(jnp.logical_not(exists[k]))
        def _(k=k, dc=dc, dr=dr):
            if dc == 0:
                target, small = (up, comp_up) if dr < 0 else (dn, comp_dn)
                for m in range(MS):
                    target[m] = jnp.zeros(target.shape[1:], jnp.float32)
                small[...] = jnp.zeros_like(small)
            else:
                for m in range(MS):
                    pack_recv[m, k - 2] = jnp.zeros(pack_recv.shape[2:], jnp.float32)
                cpack_recv[k - 2] = jnp.zeros(cpack_recv.shape[1:], jnp.float32)

    lane = lax.broadcasted_iota(jnp.int32, (rows, cols), 1)
    sub = lax.broadcasted_iota(jnp.int32, (rows, cols), 0)

    for load in loads[:2]:
        load.wait()
    mask = land[...].astype(jnp.float32)

    def place(m):
        for i in range(M):
            for c in range(2):
                own[m, pl.ds(c * M + i, rows, stride=LINE), :] = slc[m * M + i, c] * mask
        own[m, rows * LINE :, :] = jnp.zeros((own.shape[1] - rows * LINE, cols), jnp.float32)

    def pack(m):
        packed = [jnp.zeros((SUB, cols), jnp.float32)] * 2
        for block in range(PACK // SUB):
            at = block * SUB
            low = high = jnp.zeros((SUB, cols), jnp.float32)
            for r in range(rows):
                turned = pltpu.roll(own[m, r * LINE + at : r * LINE + at + SUB, :], REACH * (r + 1), 1)
                high = jnp.where((lane >= r * REACH) & (lane < (r + 1) * REACH), turned, high)
                low = jnp.where((lane >= (r + 1) * REACH) & (lane < (r + 2) * REACH), turned, low)
            here = (lane >= block * strip) & (lane < (block + 1) * strip)
            for side, value in enumerate((pltpu.roll(low, (block * strip - REACH) % cols, 1), high)):
                if side and block:
                    value = pltpu.roll(value, block * strip, 1)
                packed[side] = jnp.where(here, value, packed[side])
        for side in range(2):
            pack_send[m, side] = packed[side]

    def mirror(k):
        dr, dc = AROUND[k]
        return AROUND.index((-dr, -dc))

    def fresh_pair(m, k, sending):
        dr, dc = AROUND[k]
        back = mirror(k)
        slot = back if sending else k
        if dc == 0:
            source = own.at[m, pl.ds(0 if dr < 0 else rows * LINE - EDGE, EDGE)]
            target = (up if AROUND[slot][0] < 0 else dn).at[m, pl.ds(0, EDGE)]
        else:
            source = pack_send.at[m, 0 if dc < 0 else 1]
            target = pack_recv.at[m, slot - 2]
        return pltpu.make_async_remote_copy(
            src_ref=source,
            dst_ref=target,
            send_sem=send_a.at[k],
            recv_sem=recv_a.at[m, slot],
            device_id=(my_row + dr, my_col + dc),
            device_id_type=mesh_id,
        )

    def each_around(action, which=range(len(AROUND))):
        for k in which:

            @pl.when(exists[k])
            def _(k=k):
                action(k)

    beside, strips = range(2), range(2, len(AROUND))
    outward = (2, 4, 5, 7, 3, 6, 0, 1)
    place(0)
    pack(0)
    pl.semaphore_wait(barrier, expected)
    each_around(lambda k: fresh_pair(0, k, True).start(), outward)
    next_wave()

    k_at = lax.broadcasted_iota(jnp.int32, (cols, cols), 0)
    n_at = lax.broadcasted_iota(jnp.int32, (cols, cols), 1)
    near = jnp.where((k_at - n_at <= REACH) & (n_at - k_at <= REACH), 1.0, 0.0).astype(jnp.bfloat16)
    w_main[0:cols, :] = near
    w_main[cols:, :] = near
    line_of = k_at // REACH
    inner = k_at - line_of * REACH
    for side in range(2):
        touches = (n_at <= inner) if side == 0 else (n_at >= inner + cols - REACH)
        line = jnp.where(touches, line_of, -1)
        for r in range(rows):
            first = rows - REACH + r
            w_halo[side * cols : (side + 1) * cols, r * cols : (r + 1) * cols] = jnp.where(
                (line >= first) & (line < first + WIN), 1.0, 0.0
            ).astype(jnp.bfloat16)

    lines_total = WIN + rows - 1

    def gather_halo(parts):
        sides = []
        for side in range(2):
            a, b, c = (parts(side * 3 + j) for j in range(3))
            which = lax.broadcasted_iota(jnp.int32, a.shape, 1)
            sides.append(jnp.where(which < strip, a, jnp.where(which < 2 * strip, b, c)))
        return sides

    def line_tile(m, e, c, first):
        if e < REACH:
            buffer, at = up, SKIP + e * LINE
        elif e < REACH + rows:
            buffer, at = own, (e - REACH) * LINE
        else:
            buffer, at = dn, (e - REACH - rows) * LINE
        at += c * M + first
        return buffer[m, at : at + SUB, :]

    def halo_tile(m, side, c, first):
        at = c * M + first
        return halo[m, side, at : at + SUB, :]

    def real_part(a, b, x, y):
        return a * x + b * y

    def imag_part(a, b, x, y):
        return b * x - a * y

    def operands(tile, unit):
        lead = [tile(c, 0) for c in range(2)]
        if unit == 0:
            return lead, lead
        if unit < SUB // 2:
            return lead, [pltpu.roll(v, SUB - unit, 0) for v in lead]
        if unit == SUB // 2:
            left, right = [], []
            for c in range(2):
                mid, late = tile(c, SUB // 2), tile(c, SUB - M + 5)
                left.append(jnp.where(sub < 4, lead[c], jnp.where(sub == 4, mid, late)))
                right.append(jnp.where(sub < 4, mid, jnp.where(sub == 4, tile(c, 5), late)))
            return left, right
        return lead, None

    def products(tile, row_tile, unit):
        (a, b), other = operands(tile, unit)
        if unit == 0:
            return a * a + b * b, None
        if other is None:
            image = M - 3 + unit - SUB // 2
            x, y = (jnp.broadcast_to(row_tile(c, image), (SUB, cols)) for c in range(2))
        else:
            x, y = other
        return real_part(a, b, x, y), imag_part(a, b, x, y)

    def tile_of(m, e):
        if e < lines_total:
            return functools.partial(line_tile, m, e)
        return functools.partial(halo_tile, m, e - lines_total)

    def row_of(m, e):
        tile = tile_of(m, e)
        return lambda c, image: tile(c, image)[0:1]

    def emit_side(unit, side, value):
        high, low = split(value)
        at = slice(unit * 2 * SUB, (unit + 1) * 2 * SUB)
        hbuf[0, at, side * cols : (side + 1) * cols] = high
        hbuf[1, at, side * cols : (side + 1) * cols] = low

    def edges(count):
        for r in range(0, rows, 2):
            band = w_halo[:, r * cols : (r + 2) * cols]
            value = jnp.dot(hbuf[0, 0:count], band, preferred_element_type=jnp.float32) + jnp.dot(
                hbuf[1, 0:count], band, preferred_element_type=jnp.float32
            )
            ebuf[r, 0:count] = value[:, 0:cols]
            ebuf[r + 1, 0:count] = value[:, cols:]

    partials = {}
    for r in range(rows):
        partials.setdefault(own_range(r, rows), len(partials))

    def keep_own(unit, lines):
        for key, value in own_sums(lines, rows).items():
            at = (unit * len(partials) + partials[key]) * 2 * SUB
            pbuf[at : at + 2 * SUB, :] = value

    def emit_lines(unit, lines, target, step):
        def partial(r):
            at = (unit * len(partials) + partials[own_range(r, rows)]) * 2 * SUB
            return pbuf[at : at + 2 * SUB, :]

        for r, total in enumerate(window_sums(lines[:REACH], lines[REACH:], partial, rows)):
            high, low = split(total)
            ybuf[unit, r * 2 * SUB : (r + 1) * 2 * SUB, 0:cols] = high
            ybuf[unit, r * 2 * SUB : (r + 1) * 2 * SUB, cols:] = low
        main = jnp.dot(ybuf[unit], w_main[...], preferred_element_type=jnp.float32)
        for r in range(rows):
            at = r * step + unit * 2 * SUB
            target[at : at + 2 * SUB, :] = (
                main[r * 2 * SUB : (r + 1) * 2 * SUB, :] + ebuf[r, unit * 2 * SUB : (unit + 1) * 2 * SUB]
            )

    def both_halves(pair):
        first, second = pair
        return jnp.concatenate([first, jnp.zeros_like(first) if second is None else second], 0)

    own_lines = range(REACH, REACH + rows)
    far_lines = [*range(REACH), *range(REACH + rows, lines_total)]

    def fresh_values(m, e, unit):
        return both_halves(products(tile_of(m, e), row_of(m, e), unit))

    def fresh_own(m):
        for unit in range(len(GROUPS)):
            keep_own(unit, [fresh_values(m, e, unit) for e in own_lines])

    def fresh_sides(m):
        for side in range(2):
            for unit in range(len(GROUPS)):
                emit_side(unit, side, fresh_values(m, lines_total + side, unit))
        edges(FRESH_ROWS)

    def fresh_far(m):
        for unit in range(len(GROUPS)):
            emit_lines(unit, [fresh_values(m, e, unit) for e in far_lines], zbuf, FRESH_STEP)

    def comp_row(e, c):
        if e < REACH:
            at = c * rows + rows - REACH + e
            return comp_up[at : at + 1, :]
        if e < REACH + rows:
            at = c * rows + e - REACH
            return comp_send[at : at + 1, :]
        if e < lines_total:
            at = c * rows + e - REACH - rows
            return comp_dn[at : at + 1, :]
        return chalo[e - lines_total, c : c + 1, :]

    def late_products(m, e, unit):
        tile = tile_of(m, e)
        x, y = (jnp.broadcast_to(comp_row(e, c), (SUB, cols)) for c in range(2))
        if unit == 0:
            a, b = tile(0, 0), tile(1, 0)
        else:
            a, b = (jnp.where(sub < 2 * SUB - M, v, tile(c, M - SUB)) for c, v in enumerate((x, y)))
        return jnp.concatenate([real_part(a, b, x, y), imag_part(a, b, x, y)], 0)

    def late_fields(m):
        for side in range(2):
            for unit in range(len(LATE)):
                emit_side(unit, side, late_products(m, lines_total + side, unit))
        edges(LATE_ROWS)
        for unit in range(len(LATE)):
            emit_lines(unit, [late_products(m, e, unit) for e in far_lines], zcbuf, LATE_STEP)

    def late_own(m):
        for unit in range(len(LATE)):
            keep_own(unit, [late_products(m, e, unit) for e in own_lines])

    def fresh_field(i, j, p):
        return zbuf[pl.ds(FIELDS[(i, j, p)], rows, stride=FRESH_STEP), :]

    def late_field(i, j, p):
        return zcbuf[pl.ds(LATE_FIELDS[(i, j, p)], rows, stride=LATE_STEP), :]

    class Coherence:
        def __init__(self):
            self.scales = {}
            self.slot = {}
            self.re = {}
            self.im = {}
            self.used = 0

        def keep(self, key, value):
            coh[self.used] = value
            self.slot[key] = self.used
            self.used += 1

        def get(self, key):
            return coh[self.slot[key]]

        def tally(self, sums, i, value, minus=False):
            if i in sums:
                sums[i] = sums[i] - value if minus else sums[i] + value
            else:
                sums[i] = -value if minus else value

        def add(self, images, pairs, field):
            for i in images:
                value = field(i, i, 0)
                scale = lax.rsqrt(jnp.maximum(value, covariance_floor))
                self.scales[i] = scale
                value = value * (scale * scale)
                self.keep((i, i), value)
                self.tally(self.re, i, value)
            for i, j in pairs:
                s = self.scales[i] * self.scales[j]
                c = field(i, j, 0) * s
                d = field(i, j, 1) * s
                self.keep((i, j, 0), c)
                self.keep((i, j, 1), c + d)
                self.keep((i, j, 2), c - d)
                self.tally(self.re, i, c)
                self.tally(self.re, j, c)
                self.tally(self.im, i, d)
                self.tally(self.im, j, d, True)

        def power(self):
            images = sorted(self.re)
            re = [self.re[i] for i in images]
            im = [self.im[i] for i in images]
            gain = None
            for step in range(ITERS):
                if step:
                    both = [x + y for x, y in zip(re, im)]
                    new_re, new_im = [], []
                    for i in images:
                        shared = first = second = None
                        for j in images:
                            if j == i:
                                continue
                            key = (i, j) if (i, j, 0) in self.slot else (j, i)
                            turn = key != (i, j)
                            c = self.get(key + (0,)) * both[j]
                            e = self.get(key + (2 if turn else 1,)) * im[j]
                            f = self.get(key + (1 if turn else 2,)) * re[j]
                            shared = c if shared is None else shared + c
                            first = e if first is None else first + e
                            second = f if second is None else second + f
                        c = self.get((i, i))
                        new_re.append((shared - first) + c * re[i])
                        new_im.append((shared - second) + c * im[i])
                    re, im = new_re, new_im
                squares = [x * x + y * y for x, y in zip(re, im)]
                while len(squares) > 1:
                    squares = [sum(squares[k + 1 : k + 2], squares[k]) for k in range(0, len(squares), 2)]
                length = jnp.sqrt(squares[0])
                if gain is not None:
                    length = length * gain
                inverse = 1.0 / jnp.maximum(length, 1.0)
                gain = inverse if gain is None else gain * inverse
            return length, gain, re, im

    def finish(m, number, length, gain, re, im):
        comp_re = comp_im = None
        for i in range(M):
            a = own[m, pl.ds(i, rows, stride=LINE), :]
            b = own[m, pl.ds(M + i, rows, stride=LINE), :]
            x = re[i] * a + im[i] * b
            y = re[i] * b - im[i] * a
            comp_re = x if comp_re is None else comp_re + x
            comp_im = y if comp_im is None else comp_im + y
        return comp_re * gain, comp_im * gain

    def put_linked(m, gain, re, im):
        factor = gain * mask
        for i in range(M):
            linked[m * M + i, 0] = re[i] * factor
            linked[m * M + i, 1] = im[i] * factor

    def share_of(number, length):
        return jnp.sum(mask * length, axis=0, keepdims=True) * (1.0 / number)

    def take_strips(m):
        each_around(lambda k: fresh_pair(m, k, False).wait_recv(), strips)
        for block in range(PACK // SUB):

            def turned(j, block=block):
                value = pack_recv[m, j]
                shift = (j % 3 - block) * strip % cols
                return pltpu.roll(value, shift, 1) if shift else value

            for side, value in enumerate(gather_halo(turned)):
                halo[m, side, block * SUB : (block + 1) * SUB, :] = value

    def take_beside(m):
        each_around(lambda k: fresh_pair(m, k, False).wait_recv(), beside)

    fresh_own(0)
    for m in range(1, MS):
        loads[1 + m].wait()
        place(m)
        pack(m)
    take_strips(0)
    for m in range(1, MS):
        each_around(lambda k, m=m: fresh_pair(m, k, True).start(), outward)
    fresh_sides(0)
    next_wave()
    take_beside(0)
    fresh_far(0)
    early = Coherence()
    early.add(range(M), PAIRS, fresh_field)
    length, gain, re, im = early.power()
    comp_re, comp_im = finish(0, M, length, gain, re, im)
    comp_send[0:rows, :] = comp_re
    comp_send[rows:, :] = comp_im

    def comp_pair(k, sending):
        dr, dc = AROUND[k]
        slot = mirror(k) if sending else k
        if dc == 0:
            source = comp_send
            target = comp_up if AROUND[slot][0] < 0 else comp_dn
        else:
            source = cpack_send.at[0 if dc < 0 else 1]
            target = cpack_recv.at[slot - 2]
        return pltpu.make_async_remote_copy(
            src_ref=source,
            dst_ref=target,
            send_sem=send_b.at[k],
            recv_sem=recv_b.at[slot],
            device_id=(my_row + dr, my_col + dc),
            device_id_type=mesh_id,
        )

    each_around(lambda k: comp_pair(k, True).start(), beside)
    for c, value in enumerate((comp_re, comp_im)):
        for side in range(2):
            total = jnp.zeros((rows, cols), jnp.float32)
            for copy in range(3):
                turned = pltpu.roll(value, REACH * side + strip * copy, 1, stride=REACH, stride_axis=0)
                first = strip * copy + sub * REACH
                total = jnp.where((lane >= first) & (lane < first + REACH), turned, total)
            cpack_send[side, c : c + 1, :] = jnp.sum(total, axis=0, keepdims=True)

    each_around(lambda k: comp_pair(k, True).start(), (2, 4, 5, 7, 3, 6))

    put_linked(0, gain, re, im)
    part[0:1] = share_of(M, length)
    last = MS - 1
    fresh_own(last)
    take_strips(last)
    fresh_sides(last)
    take_beside(last)
    fresh_far(last)
    late_own(last)
    joint = Coherence()
    joint.add(range(M), PAIRS, fresh_field)
    while len(pending) and pending[0][0] < len(offsets) - 1:
        next_wave()

    each_around(lambda k: comp_pair(k, False).wait_recv())
    for side, value in enumerate(gather_halo(lambda j: cpack_recv[j])):
        chalo[side] = value
    late_fields(last)
    joint.add([M], LATE_PAIRS, late_field)
    length, gain, re, im = joint.power()
    part[last : last + 1] = share_of(M + 1, length)
    while pending:
        next_wave()

    def reduce(count, me, device, source, buffer, sends, recvs):
        copies = []
        for step in range(1, count):
            copy = pltpu.make_async_remote_copy(
                src_ref=source,
                dst_ref=buffer.at[me],
                send_sem=sends.at[step],
                recv_sem=recvs.at[me],
                device_id=device(lax.rem(me + step, count)),
                device_id_type=mesh_id,
            )
            copy.start()
            copies.append(copy)
        buffer[me] = source[...]
        for step in range(1, count):
            other = lax.rem(me + step, count)
            pltpu.make_async_remote_copy(
                src_ref=source,
                dst_ref=buffer.at[other],
                send_sem=sends.at[step],
                recv_sem=recvs.at[other],
                device_id=device(other),
                device_id_type=mesh_id,
            ).wait_recv()
        for copy in copies:
            copy.wait_send()
        total = buffer[0]
        for other in range(1, count):
            total = total + buffer[other]
        return total

    def close_last():
        comp_re, comp_im = finish(last, M + 1, length, gain, re, im)
        comp_out[0] = comp_re
        comp_out[1] = comp_im
        put_linked(last, gain, re, im)

    def sent(k):
        dr, dc = AROUND[k]
        if dc == 0:
            source, target = own.at[:, pl.ds(0, EDGE)], up.at[:, pl.ds(0, EDGE)]
        else:
            source, target = pack_send.at[:, 0], pack_recv.at[:, 0]
        return pltpu.make_async_remote_copy(
            src_ref=source,
            dst_ref=target,
            send_sem=send_a.at[k],
            recv_sem=recv_a.at[0, k],
            device_id=(my_row + dr, my_col + dc),
            device_id_type=mesh_id,
        )

    def finish_sends():
        each_around(lambda k: sent(k).wait_send())
        each_around(lambda k: comp_pair(k, True).wait_send())

    def flips(position, count):
        steps = []
        size = 1
        while size < count:
            steps.append(size * (1 - 2 * lax.rem(position // size, 2)))
            size *= 2
        return steps

    def swapped(position, steps, mask_bits):
        for bit, step in enumerate(steps):
            if mask_bits >> bit & 1:
                position = position + step
        return position

    if direct:
        count = row_count * col_count
        row_steps, col_steps = flips(my_row, row_count), flips(my_col, col_count)

        def weight(code):
            return -bin(code // col_count).count("1") - code % col_count

        for code in sorted(range(1, count), key=weight):
            pltpu.make_async_remote_copy(
                src_ref=part,
                dst_ref=red_row.at[code],
                send_sem=send_r.at[0],
                recv_sem=recv_r.at[0],
                device_id=(
                    swapped(my_row, row_steps, code // col_count),
                    swapped(my_col, col_steps, code % col_count),
                ),
                device_id_type=mesh_id,
            ).start()
        close_last()
        finish_sends()
        everything = pltpu.make_async_remote_copy(
            src_ref=red_row.at[pl.ds(1, count - 1)],
            dst_ref=red_row.at[pl.ds(1, count - 1)],
            send_sem=send_r.at[0],
            recv_sem=recv_r.at[0],
            device_id=(swapped(my_row, row_steps, row_count - 1), swapped(my_col, col_steps, col_count - 1)),
            device_id_type=mesh_id,
        )
        everything.wait_recv()
        values = [part[...]] + [red_row[code] for code in range(1, count)]
        while len(values) > 1:
            values = [values[k] + values[k + 1] for k in range(0, len(values), 2)]
        total = values[0]
        strength[...] = total
        everything.wait_send()
    else:
        total = reduce(row_count, my_row, lambda d: (d, my_col), part, red_row, send_r, recv_r)
        part2 = red_col.at[col_count]
        part2[...] = total
        total = reduce(col_count, my_col, lambda d: (my_row, d), part2, red_col, send_r.at[pl.ds(row_count, col_count)], recv_r.at[pl.ds(row_count, col_count)])
        strength[...] = total
        close_last()
        finish_sends()


def closing(pixels, linked_in, comp_in, total, linked, comp, strength, scalars, sems):
    copies = [
        pltpu.make_async_copy(linked_in, linked, sems.at[0]),
        pltpu.make_async_copy(comp_in, comp, sems.at[1]),
        pltpu.make_async_copy(scalars, strength, sems.at[2]),
    ]
    for copy in copies[:2]:
        copy.start()
    for m in range(MS):
        scalars[m] = jnp.sum(total[m : m + 1]) / pixels
    copies[2].start()
    for copy in copies:
        copy.wait()


def shards(slc_stack, land_mask):
    rows, cols = land_mask.shape
    row_count, col_count = lax.axis_size("row"), lax.axis_size("col")
    f32, bf16 = jnp.float32, jnp.bfloat16
    vmem = pl.BlockSpec(memory_space=pltpu.VMEM)
    dma = pltpu.SemaphoreType.DMA
    hbm = pl.BlockSpec(memory_space=pltpu.HBM)
    devices = row_count * col_count
    direct = devices <= 64 and row_count & (row_count - 1) == 0 and col_count & (col_count - 1) == 0
    peers = devices if direct else row_count
    linked_shape = jax.ShapeDtypeStruct(slc_stack.shape, f32)
    comp_shape = jax.ShapeDtypeStruct((2, rows, cols), f32)
    linked, comp, total = pl.pallas_call(
        functools.partial(kernel, row_count, col_count, direct),
        out_shape=(linked_shape, comp_shape, jax.ShapeDtypeStruct((MS, cols), f32)),
        in_specs=[hbm, hbm],
        out_specs=(vmem, vmem, vmem),
        scratch_shapes=[
            pltpu.VMEM(slc_stack.shape, f32),
            pltpu.VMEM((rows, cols), jnp.int32),
            pltpu.VMEM((MS, rows * LINE + SUB, cols), f32),
            pltpu.VMEM((MS, EDGE + SUB, cols), f32),
            pltpu.VMEM((MS, EDGE + SUB, cols), f32),
            pltpu.VMEM((MS, 2, SUB, cols), f32),
            pltpu.VMEM((MS, 6, SUB, cols), f32),
            pltpu.VMEM((MS, 2, PACK, cols), f32),
            pltpu.VMEM((2 * rows, cols), f32),
            pltpu.VMEM((2 * rows, cols), f32),
            pltpu.VMEM((2 * rows, cols), f32),
            pltpu.VMEM((2, 2, cols), f32),
            pltpu.VMEM((6, 2, cols), f32),
            pltpu.VMEM((2, 2, cols), f32),
            pltpu.VMEM((2 * cols, cols), bf16),
            pltpu.VMEM((2 * cols, rows * cols), bf16),
            pltpu.VMEM((len(GROUPS) * rows * 2 * SUB, cols), f32),
            pltpu.VMEM((len(GROUPS), rows * 2 * SUB, 2 * cols), bf16),
            pltpu.VMEM((2, FRESH_ROWS, 2 * cols), bf16),
            pltpu.VMEM((rows, FRESH_ROWS, cols), f32),
            pltpu.VMEM((rows * FRESH_STEP, cols), f32),
            pltpu.VMEM((rows * LATE_STEP, cols), f32),
            pltpu.VMEM((SLOTS, rows, cols), f32),
            pltpu.VMEM((MS, cols), f32),
            pltpu.VMEM((peers, MS, cols), f32),
            pltpu.VMEM((col_count + 1, MS, cols), f32),
            dma((MS + 1,)),
            pltpu.SemaphoreType.REGULAR((max(1, len(waves(row_count, col_count))),)),
            dma((len(AROUND),)),
            dma((MS, len(AROUND))),
            dma((len(AROUND),)),
            dma((len(AROUND),)),
            dma((1 if direct else row_count + col_count,)),
            dma((1 if direct else row_count + col_count,)),
        ],
        compiler_params=pltpu.CompilerParams(collective_id=0, has_side_effects=True, vmem_limit_bytes=16 << 20),
        name="linker",
    )(*(pltpu.with_memory_space_constraint(x, pltpu.HBM) for x in (slc_stack, land_mask)))
    return pl.pallas_call(
        functools.partial(closing, rows * cols * devices),
        out_shape=(linked_shape, comp_shape, jax.ShapeDtypeStruct((MS,), f32)),
        in_specs=[vmem, vmem, vmem],
        out_specs=(hbm, hbm, hbm),
        scratch_shapes=[pltpu.SMEM((MS,), f32), dma((3,))],
        compiler_params=pltpu.CompilerParams(vmem_limit_bytes=4 << 20),
        name="closing",
    )(linked, comp, total)


def solution(mesh):
    return jax.shard_map(
        shards,
        mesh=mesh,
        in_specs=(P(None, None, "row", "col"), P("row", "col")),
        out_specs=(P(None, None, "row", "col"), P(None, "row", "col"), P()),
        check_vma=False,
    )
```

```python
import functools

import jax
import jax.numpy as jnp
from jax import lax
from jax.experimental import pallas as pl
from jax.experimental.pallas import tpu as pltpu
from jax.sharding import PartitionSpec as P

M = 10
MS = 2
WIN = 11
ITERS = 4
REACH = WIN // 2
SUB = 8

covariance_floor = 8.0

AROUND = ((-1, 0), (1, 0), (-1, -1), (0, -1), (1, -1), (-1, 1), (0, 1), (1, 1))
LINE = 2 * M
EDGE = -(-REACH * LINE // SUB) * SUB
SKIP = EDGE - REACH * LINE
PACK = -(-LINE // SUB) * SUB


def pair_groups():
    groups = [[(s, (s + lag) % SUB) for s in range(SUB)] for lag in range(SUB // 2)]
    half = SUB // 2
    groups.append([(s, s + half) for s in range(half)] + [(M - 2, M - 1), (M - 2, M - 2), (M - 1, M - 1)])
    groups.append([(s, M - 2) for s in range(SUB)])
    groups.append([(s, M - 1) for s in range(SUB)])
    return groups


def field_rows(groups):
    table = {}
    for unit, group in enumerate(groups):
        for lane, (i, j) in enumerate(group):
            for part in range(1 if i == j else 2):
                table[(i, j, part)] = unit * 2 * SUB + part * SUB + lane
    return table


GROUPS = pair_groups()
LATE = [[(s, M) for s in range(SUB)], [(M, M)] * (2 * SUB - M) + [(s, M) for s in range(SUB, M)]]
FIELDS = field_rows(GROUPS)
LATE_FIELDS = field_rows(LATE)
PAIRS = [(i, j) for i, j, part in FIELDS if part == 1]
LATE_PAIRS = [(i, j) for i, j, part in LATE_FIELDS if part == 1]
FRESH_ROWS = len(GROUPS) * 2 * SUB
LATE_ROWS = len(LATE) * 2 * SUB
FRESH_STEP = FRESH_ROWS + 4
LATE_STEP = LATE_ROWS + 4
SLOTS = 3 * (len(PAIRS) + len(LATE_PAIRS)) + M + 1


def own_range(r, rows):
    return max(r, REACH), min(r + WIN, REACH + rows)


def own_sums(lines, rows):
    core = lines[rows - 1 - REACH]
    for e in range(rows, WIN):
        core = core + lines[e - REACH]
    starts = {rows - 1: core}
    for e in range(rows - 2, REACH - 1, -1):
        starts[e] = starts[e + 1] + lines[e - REACH]
    tails = {WIN: None}
    for e in range(WIN, REACH + rows):
        tails[e + 1] = lines[e - REACH] if tails[e] is None else tails[e] + lines[e - REACH]
    sums = {}
    for r in range(rows):
        start, stop = own_range(r, rows)
        if (start, stop) not in sums:
            tail = tails[stop]
            sums[(start, stop)] = starts[start] if tail is None else starts[start] + tail
    return sums


def window_sums(above, below, partial, rows):
    lead = {REACH: None}
    for e in range(REACH - 1, -1, -1):
        lead[e] = above[e] if lead[e + 1] is None else lead[e + 1] + above[e]
    trail = {0: None}
    for e in range(REACH):
        trail[e + 1] = below[e] if trail[e] is None else trail[e] + below[e]
    sums = []
    for r in range(rows):
        total = partial(r)
        for extra in (lead[min(r, REACH)], trail[max(0, r + WIN - REACH - rows)]):
            if extra is not None:
                total = total + extra
        sums.append(total)
    return sums


def split(value):
    high = value.astype(jnp.bfloat16)
    low = (value - high.astype(jnp.float32)).astype(jnp.bfloat16)
    return high, low


def waves(row_count, col_count):
    offsets = []
    known = 1
    while known < max(row_count, col_count) - 1:
        offsets.append(known)
        known *= 2
    return offsets


def kernel(
    row_count,
    col_count,
    direct,
    slc_hbm,
    land_hbm,
    linked,
    comp_out,
    strength,
    slc,
    land,
    own,
    up,
    dn,
    pack_send,
    pack_recv,
    halo,
    comp_send,
    comp_up,
    comp_dn,
    cpack_send,
    cpack_recv,
    chalo,
    w_main,
    w_halo,
    pbuf,
    ybuf,
    hbuf,
    ebuf,
    zbuf,
    zcbuf,
    coh,
    part,
    red_row,
    red_col,
    load_sem,
    ready,
    send_a,
    recv_a,
    send_b,
    recv_b,
    send_r,
    recv_r,
):
    rows, cols = land.shape
    my_row = lax.axis_index("row")
    my_col = lax.axis_index("col")
    strip = rows * REACH
    mesh_id = pl.DeviceIdType.MESH
    loads = [
        pltpu.make_async_copy(land_hbm, land, load_sem.at[MS]),
    ] + [
        pltpu.make_async_copy(slc_hbm.at[pl.ds(m * M, M)], slc.at[pl.ds(m * M, M)], load_sem.at[m]) for m in range(MS)
    ]
    for load in loads:
        load.start()

    def existing(dr, dc, far=1):
        ok = None
        for pos, step, count in ((my_row, dr, row_count), (my_col, dc, col_count)):
            if step:
                here = (pos >= far) if step < 0 else (pos < count - far)
                ok = here if ok is None else jnp.logical_and(ok, here)
        return ok

    exists = [existing(dr, dc) for dr, dc in AROUND]

    def greet(semaphore, far):
        expected = jnp.int32(0)
        for dr, dc in sorted(AROUND, key=lambda step: -abs(step[0]) - abs(step[1])):
            if (dr and far >= row_count) or (dc and far >= col_count):
                continue
            there = existing(dr, dc, far)

            @pl.when(there)
            def _(dr=dr, dc=dc):
                pl.semaphore_signal(
                    semaphore,
                    inc=1,
                    device_id=(my_row + dr * far, my_col + dc * far),
                    device_id_type=mesh_id,
                )

            expected = expected + there.astype(jnp.int32)
        return expected

    barrier = pltpu.get_barrier_semaphore()
    expected = greet(barrier, 1)
    offsets = waves(row_count, col_count)
    pending = []

    def next_wave():
        if pending:
            index, count = pending.pop()
            pl.semaphore_wait(ready.at[index], count)
            index += 1
        else:
            index = 0
        if index < len(offsets):
            pending.append((index, greet(ready.at[index], offsets[index])))

    for k, (dr, dc) in enumerate(AROUND):

        @pl.when(jnp.logical_not(exists[k]))
        def _(k=k, dc=dc, dr=dr):
            if dc == 0:
                target, small = (up, comp_up) if dr < 0 else (dn, comp_dn)
                for m in range(MS):
                    target[m] = jnp.zeros(target.shape[1:], jnp.float32)
                small[...] = jnp.zeros_like(small)
            else:
                for m in range(MS):
                    pack_recv[m, k - 2] = jnp.zeros(pack_recv.shape[2:], jnp.float32)
                cpack_recv[k - 2] = jnp.zeros(cpack_recv.shape[1:], jnp.float32)

    lane = lax.broadcasted_iota(jnp.int32, (rows, cols), 1)
    sub = lax.broadcasted_iota(jnp.int32, (rows, cols), 0)

    for load in loads[:2]:
        load.wait()
    mask = land[...].astype(jnp.float32)

    def place(m):
        for i in range(M):
            for c in range(2):
                own[m, pl.ds(c * M + i, rows, stride=LINE), :] = slc[m * M + i, c] * mask
        own[m, rows * LINE :, :] = jnp.zeros((own.shape[1] - rows * LINE, cols), jnp.float32)

    def pack(m):
        packed = [jnp.zeros((SUB, cols), jnp.float32)] * 2
        for block in range(PACK // SUB):
            at = block * SUB
            low = high = jnp.zeros((SUB, cols), jnp.float32)
            for r in range(rows):
                turned = pltpu.roll(own[m, r * LINE + at : r * LINE + at + SUB, :], REACH * (r + 1), 1)
                high = jnp.where((lane >= r * REACH) & (lane < (r + 1) * REACH), turned, high)
                low = jnp.where((lane >= (r + 1) * REACH) & (lane < (r + 2) * REACH), turned, low)
            here = (lane >= block * strip) & (lane < (block + 1) * strip)
            for side, value in enumerate((pltpu.roll(low, (block * strip - REACH) % cols, 1), high)):
                if side and block:
                    value = pltpu.roll(value, block * strip, 1)
                packed[side] = jnp.where(here, value, packed[side])
        for side in range(2):
            pack_send[m, side] = packed[side]

    def mirror(k):
        dr, dc = AROUND[k]
        return AROUND.index((-dr, -dc))

    def fresh_pair(m, k, sending):
        dr, dc = AROUND[k]
        back = mirror(k)
        slot = back if sending else k
        if dc == 0:
            source = own.at[m, pl.ds(0 if dr < 0 else rows * LINE - EDGE, EDGE)]
            target = (up if AROUND[slot][0] < 0 else dn).at[m, pl.ds(0, EDGE)]
        else:
            source = pack_send.at[m, 0 if dc < 0 else 1]
            target = pack_recv.at[m, slot - 2]
        return pltpu.make_async_remote_copy(
            src_ref=source,
            dst_ref=target,
            send_sem=send_a.at[k],
            recv_sem=recv_a.at[m, slot],
            device_id=(my_row + dr, my_col + dc),
            device_id_type=mesh_id,
        )

    def each_around(action, which=range(len(AROUND))):
        for k in which:

            @pl.when(exists[k])
            def _(k=k):
                action(k)

    beside, strips = range(2), range(2, len(AROUND))
    outward = (2, 4, 5, 7, 3, 6, 0, 1)
    place(0)
    pack(0)
    pl.semaphore_wait(barrier, expected)
    each_around(lambda k: fresh_pair(0, k, True).start(), outward)
    next_wave()

    k_at = lax.broadcasted_iota(jnp.int32, (cols, cols), 0)
    n_at = lax.broadcasted_iota(jnp.int32, (cols, cols), 1)
    near = jnp.where((k_at - n_at <= REACH) & (n_at - k_at <= REACH), 1.0, 0.0).astype(jnp.bfloat16)
    w_main[0:cols, :] = near
    w_main[cols:, :] = near
    line_of = k_at // REACH
    inner = k_at - line_of * REACH
    for side in range(2):
        touches = (n_at <= inner) if side == 0 else (n_at >= inner + cols - REACH)
        line = jnp.where(touches, line_of, -1)
        for r in range(rows):
            first = rows - REACH + r
            w_halo[side * cols : (side + 1) * cols, r * cols : (r + 1) * cols] = jnp.where(
                (line >= first) & (line < first + WIN), 1.0, 0.0
            ).astype(jnp.bfloat16)

    lines_total = WIN + rows - 1

    def gather_halo(parts):
        sides = []
        for side in range(2):
            a, b, c = (parts(side * 3 + j) for j in range(3))
            which = lax.broadcasted_iota(jnp.int32, a.shape, 1)
            sides.append(jnp.where(which < strip, a, jnp.where(which < 2 * strip, b, c)))
        return sides

    def line_tile(m, e, c, first):
        if e < REACH:
            buffer, at = up, SKIP + e * LINE
        elif e < REACH + rows:
            buffer, at = own, (e - REACH) * LINE
        else:
            buffer, at = dn, (e - REACH - rows) * LINE
        at += c * M + first
        return buffer[m, at : at + SUB, :]

    def halo_tile(m, side, c, first):
        at = c * M + first
        return halo[m, side, at : at + SUB, :]

    def real_part(a, b, x, y):
        return a * x + b * y

    def imag_part(a, b, x, y):
        return b * x - a * y

    def operands(tile, unit):
        lead = [tile(c, 0) for c in range(2)]
        if unit == 0:
            return lead, lead
        if unit < SUB // 2:
            return lead, [pltpu.roll(v, SUB - unit, 0) for v in lead]
        if unit == SUB // 2:
            left, right = [], []
            for c in range(2):
                mid, late = tile(c, SUB // 2), tile(c, SUB - M + 5)
                left.append(jnp.where(sub < 4, lead[c], jnp.where(sub == 4, mid, late)))
                right.append(jnp.where(sub < 4, mid, jnp.where(sub == 4, tile(c, 5), late)))
            return left, right
        return lead, None

    def products(tile, row_tile, unit):
        (a, b), other = operands(tile, unit)
        if unit == 0:
            return a * a + b * b, None
        if other is None:
            image = M - 3 + unit - SUB // 2
            x, y = (jnp.broadcast_to(row_tile(c, image), (SUB, cols)) for c in range(2))
        else:
            x, y = other
        return real_part(a, b, x, y), imag_part(a, b, x, y)

    def tile_of(m, e):
        if e < lines_total:
            return functools.partial(line_tile, m, e)
        return functools.partial(halo_tile, m, e - lines_total)

    def row_of(m, e):
        tile = tile_of(m, e)
        return lambda c, image: tile(c, image)[0:1]

    def emit_side(unit, side, value, count):
        high, low = split(value)
        at = unit * 2 * SUB
        hbuf[at : at + 2 * SUB, side * cols : (side + 1) * cols] = high
        hbuf[count + at : count + at + 2 * SUB, side * cols : (side + 1) * cols] = low

    def edges(count):
        for r in range(0, rows, 2):
            band = w_halo[:, r * cols : (r + 2) * cols]
            value = jnp.dot(hbuf[0 : 2 * count], band, preferred_element_type=jnp.float32)
            value = value[0:count] + value[count:]
            ebuf[r, 0:count] = value[:, 0:cols]
            ebuf[r + 1, 0:count] = value[:, cols:]

    partials = {}
    for r in range(rows):
        partials.setdefault(own_range(r, rows), len(partials))

    def keep_own(unit, lines):
        for key, value in own_sums(lines, rows).items():
            at = (unit * len(partials) + partials[key]) * 2 * SUB
            pbuf[at : at + 2 * SUB, :] = value

    def emit_lines(unit, lines):
        def partial(r):
            at = (unit * len(partials) + partials[own_range(r, rows)]) * 2 * SUB
            return pbuf[at : at + 2 * SUB, :]

        for r, total in enumerate(window_sums(lines[:REACH], lines[REACH:], partial, rows)):
            high, low = split(total)
            ybuf[unit, r * 2 * SUB : (r + 1) * 2 * SUB, 0:cols] = high
            ybuf[unit, r * 2 * SUB : (r + 1) * 2 * SUB, cols:] = low

    def emit_main(unit, main, target, step):
        for r in range(rows):
            at = r * step + unit * 2 * SUB
            target[at : at + 2 * SUB, :] = (
                main[r * 2 * SUB : (r + 1) * 2 * SUB, :] + ebuf[r, unit * 2 * SUB : (unit + 1) * 2 * SUB]
            )

    def both_halves(pair):
        first, second = pair
        return jnp.concatenate([first, jnp.zeros_like(first) if second is None else second], 0)

    own_lines = range(REACH, REACH + rows)
    far_lines = [*range(REACH), *range(REACH + rows, lines_total)]

    def fresh_values(m, e, unit):
        return both_halves(products(tile_of(m, e), row_of(m, e), unit))

    def fresh_own(m):
        for unit in range(len(GROUPS)):
            keep_own(unit, [fresh_values(m, e, unit) for e in own_lines])

    def fresh_sides(m):
        for side in range(2):
            for unit in range(len(GROUPS)):
                emit_side(unit, side, fresh_values(m, lines_total + side, unit), FRESH_ROWS)
        edges(FRESH_ROWS)

    def fresh_far(m):
        for unit in range(len(GROUPS)):
            emit_lines(unit, [fresh_values(m, e, unit) for e in far_lines])
            main = jnp.dot(ybuf[unit], w_main[...], preferred_element_type=jnp.float32)
            emit_main(unit, main, zbuf, FRESH_STEP)

    def comp_row(e, c):
        if e < REACH:
            at = c * rows + rows - REACH + e
            return comp_up[at : at + 1, :]
        if e < REACH + rows:
            at = c * rows + e - REACH
            return comp_send[at : at + 1, :]
        if e < lines_total:
            at = c * rows + e - REACH - rows
            return comp_dn[at : at + 1, :]
        return chalo[e - lines_total, c : c + 1, :]

    def late_products(m, e, unit):
        tile = tile_of(m, e)
        x, y = (jnp.broadcast_to(comp_row(e, c), (SUB, cols)) for c in range(2))
        if unit == 0:
            a, b = tile(0, 0), tile(1, 0)
        else:
            a, b = (jnp.where(sub < 2 * SUB - M, v, tile(c, M - SUB)) for c, v in enumerate((x, y)))
        return jnp.concatenate([real_part(a, b, x, y), imag_part(a, b, x, y)], 0)

    def late_fields(m):
        for side in range(2):
            for unit in range(len(LATE)):
                emit_side(unit, side, late_products(m, lines_total + side, unit), LATE_ROWS)
        edges(LATE_ROWS)
        for unit in range(len(LATE)):
            emit_lines(unit, [late_products(m, e, unit) for e in far_lines])
        size = rows * 2 * SUB
        main = jnp.dot(
            ybuf[0 : len(LATE)].reshape(len(LATE) * size, 2 * cols), w_main[...], preferred_element_type=jnp.float32
        )
        for unit in range(len(LATE)):
            emit_main(unit, main[unit * size : (unit + 1) * size], zcbuf, LATE_STEP)

    def late_own(m):
        for unit in range(len(LATE)):
            keep_own(unit, [late_products(m, e, unit) for e in own_lines])

    def fresh_field(i, j, p):
        return zbuf[pl.ds(FIELDS[(i, j, p)], rows, stride=FRESH_STEP), :]

    def late_field(i, j, p):
        return zcbuf[pl.ds(LATE_FIELDS[(i, j, p)], rows, stride=LATE_STEP), :]

    class Coherence:
        def __init__(self):
            self.scales = {}
            self.slot = {}
            self.re = {}
            self.im = {}
            self.used = 0

        def keep(self, key, value):
            coh[self.used] = value
            self.slot[key] = self.used
            self.used += 1

        def get(self, key):
            return coh[self.slot[key]]

        def tally(self, sums, i, value, minus=False):
            if i in sums:
                sums[i] = sums[i] - value if minus else sums[i] + value
            else:
                sums[i] = -value if minus else value

        def add(self, images, pairs, field):
            for i in images:
                value = field(i, i, 0)
                scale = lax.rsqrt(jnp.maximum(value, covariance_floor))
                self.scales[i] = scale
                value = value * (scale * scale)
                self.keep((i, i), value)
                self.tally(self.re, i, value)
            for i, j in pairs:
                s = self.scales[i] * self.scales[j]
                c = field(i, j, 0) * s
                d = field(i, j, 1) * s
                self.keep((i, j, 0), c)
                self.keep((i, j, 1), c + d)
                self.keep((i, j, 2), c - d)
                self.tally(self.re, i, c)
                self.tally(self.re, j, c)
                self.tally(self.im, i, d)
                self.tally(self.im, j, d, True)

        def power(self):
            images = sorted(self.re)
            re = [self.re[i] for i in images]
            im = [self.im[i] for i in images]
            gain = None
            for step in range(ITERS):
                if step:
                    both = [x + y for x, y in zip(re, im)]
                    new_re, new_im = [], []
                    for i in images:
                        shared = first = second = None
                        for j in images:
                            if j == i:
                                continue
                            key = (i, j) if (i, j, 0) in self.slot else (j, i)
                            turn = key != (i, j)
                            c = self.get(key + (0,)) * both[j]
                            e = self.get(key + (2 if turn else 1,)) * im[j]
                            f = self.get(key + (1 if turn else 2,)) * re[j]
                            shared = c if shared is None else shared + c
                            first = e if first is None else first + e
                            second = f if second is None else second + f
                        c = self.get((i, i))
                        new_re.append((shared - first) + c * re[i])
                        new_im.append((shared - second) + c * im[i])
                    re, im = new_re, new_im
                squares = [x * x + y * y for x, y in zip(re, im)]
                while len(squares) > 1:
                    squares = [sum(squares[k + 1 : k + 2], squares[k]) for k in range(0, len(squares), 2)]
                length = jnp.sqrt(squares[0])
                if gain is not None:
                    length = length * gain
                inverse = 1.0 / jnp.maximum(length, 1.0)
                gain = inverse if gain is None else gain * inverse
            return length, gain, re, im

    def finish(m, number, length, gain, re, im):
        comp_re = comp_im = None
        for i in range(M):
            a = own[m, pl.ds(i, rows, stride=LINE), :]
            b = own[m, pl.ds(M + i, rows, stride=LINE), :]
            x = re[i] * a + im[i] * b
            y = re[i] * b - im[i] * a
            comp_re = x if comp_re is None else comp_re + x
            comp_im = y if comp_im is None else comp_im + y
        return comp_re * gain, comp_im * gain

    def put_linked(m, gain, re, im):
        factor = gain * mask
        for i in range(M):
            linked[m * M + i, 0] = re[i] * factor
            linked[m * M + i, 1] = im[i] * factor

    def share_of(number, length):
        return jnp.sum(mask * length, axis=0, keepdims=True) * (1.0 / number)

    def take_strips(m):
        each_around(lambda k: fresh_pair(m, k, False).wait_recv(), strips)
        for block in range(PACK // SUB):

            def turned(j, block=block):
                value = pack_recv[m, j]
                shift = (j % 3 - block) * strip % cols
                return pltpu.roll(value, shift, 1) if shift else value

            for side, value in enumerate(gather_halo(turned)):
                halo[m, side, block * SUB : (block + 1) * SUB, :] = value

    def take_beside(m):
        each_around(lambda k: fresh_pair(m, k, False).wait_recv(), beside)

    fresh_own(0)
    for m in range(1, MS):
        loads[1 + m].wait()
        place(m)
        pack(m)
    take_strips(0)
    for m in range(1, MS):
        each_around(lambda k, m=m: fresh_pair(m, k, True).start(), outward)
    fresh_sides(0)
    next_wave()
    take_beside(0)
    fresh_far(0)
    early = Coherence()
    early.add(range(M), PAIRS, fresh_field)
    length, gain, re, im = early.power()
    comp_re, comp_im = finish(0, M, length, gain, re, im)
    comp_send[0:rows, :] = comp_re
    comp_send[rows:, :] = comp_im

    def comp_pair(k, sending):
        dr, dc = AROUND[k]
        slot = mirror(k) if sending else k
        if dc == 0:
            source = comp_send
            target = comp_up if AROUND[slot][0] < 0 else comp_dn
        else:
            source = cpack_send.at[0 if dc < 0 else 1]
            target = cpack_recv.at[slot - 2]
        return pltpu.make_async_remote_copy(
            src_ref=source,
            dst_ref=target,
            send_sem=send_b.at[k],
            recv_sem=recv_b.at[slot],
            device_id=(my_row + dr, my_col + dc),
            device_id_type=mesh_id,
        )

    each_around(lambda k: comp_pair(k, True).start(), beside)
    for c, value in enumerate((comp_re, comp_im)):
        for side in range(2):
            total = jnp.zeros((rows, cols), jnp.float32)
            for copy in range(3):
                turned = pltpu.roll(value, REACH * side + strip * copy, 1, stride=REACH, stride_axis=0)
                first = strip * copy + sub * REACH
                total = jnp.where((lane >= first) & (lane < first + REACH), turned, total)
            cpack_send[side, c : c + 1, :] = jnp.sum(total, axis=0, keepdims=True)

    each_around(lambda k: comp_pair(k, True).start(), (2, 4, 5, 7, 3, 6))

    put_linked(0, gain, re, im)
    part[0:1] = share_of(M, length)
    last = MS - 1
    fresh_own(last)
    take_strips(last)
    fresh_sides(last)
    take_beside(last)
    fresh_far(last)
    late_own(last)
    joint = Coherence()
    joint.add(range(M), PAIRS, fresh_field)
    while len(pending) and pending[0][0] < len(offsets) - 1:
        next_wave()

    each_around(lambda k: comp_pair(k, False).wait_recv())
    for side, value in enumerate(gather_halo(lambda j: cpack_recv[j])):
        chalo[side] = value
    late_fields(last)
    joint.add([M], LATE_PAIRS, late_field)
    length, gain, re, im = joint.power()
    part[last : last + 1] = share_of(M + 1, length)
    while pending:
        next_wave()

    def reduce(count, me, device, source, buffer, sends, recvs):
        copies = []
        for step in range(1, count):
            copy = pltpu.make_async_remote_copy(
                src_ref=source,
                dst_ref=buffer.at[me],
                send_sem=sends.at[step],
                recv_sem=recvs.at[me],
                device_id=device(lax.rem(me + step, count)),
                device_id_type=mesh_id,
            )
            copy.start()
            copies.append(copy)
        buffer[me] = source[...]
        for step in range(1, count):
            other = lax.rem(me + step, count)
            pltpu.make_async_remote_copy(
                src_ref=source,
                dst_ref=buffer.at[other],
                send_sem=sends.at[step],
                recv_sem=recvs.at[other],
                device_id=device(other),
                device_id_type=mesh_id,
            ).wait_recv()
        for copy in copies:
            copy.wait_send()
        total = buffer[0]
        for other in range(1, count):
            total = total + buffer[other]
        return total

    def close_last():
        comp_re, comp_im = finish(last, M + 1, length, gain, re, im)
        comp_out[0] = comp_re
        comp_out[1] = comp_im
        put_linked(last, gain, re, im)

    def sent(k):
        dr, dc = AROUND[k]
        if dc == 0:
            source, target = own.at[:, pl.ds(0, EDGE)], up.at[:, pl.ds(0, EDGE)]
        else:
            source, target = pack_send.at[:, 0], pack_recv.at[:, 0]
        return pltpu.make_async_remote_copy(
            src_ref=source,
            dst_ref=target,
            send_sem=send_a.at[k],
            recv_sem=recv_a.at[0, k],
            device_id=(my_row + dr, my_col + dc),
            device_id_type=mesh_id,
        )

    def finish_sends():
        each_around(lambda k: sent(k).wait_send())
        each_around(lambda k: comp_pair(k, True).wait_send())

    def flips(position, count):
        steps = []
        size = 1
        while size < count:
            steps.append(size * (1 - 2 * lax.rem(position // size, 2)))
            size *= 2
        return steps

    def swapped(position, steps, mask_bits):
        for bit, step in enumerate(steps):
            if mask_bits >> bit & 1:
                position = position + step
        return position

    if direct:
        count = row_count * col_count
        row_steps, col_steps = flips(my_row, row_count), flips(my_col, col_count)

        def weight(code):
            return -bin(code // col_count).count("1") - code % col_count

        for code in sorted(range(1, count), key=weight):
            pltpu.make_async_remote_copy(
                src_ref=part,
                dst_ref=red_row.at[code],
                send_sem=send_r.at[0],
                recv_sem=recv_r.at[0],
                device_id=(
                    swapped(my_row, row_steps, code // col_count),
                    swapped(my_col, col_steps, code % col_count),
                ),
                device_id_type=mesh_id,
            ).start()
        close_last()
        finish_sends()
        everything = pltpu.make_async_remote_copy(
            src_ref=red_row.at[pl.ds(1, count - 1)],
            dst_ref=red_row.at[pl.ds(1, count - 1)],
            send_sem=send_r.at[0],
            recv_sem=recv_r.at[0],
            device_id=(swapped(my_row, row_steps, row_count - 1), swapped(my_col, col_steps, col_count - 1)),
            device_id_type=mesh_id,
        )
        everything.wait_recv()
        values = [part[...]] + [red_row[code] for code in range(1, count)]
        while len(values) > 1:
            values = [values[k] + values[k + 1] for k in range(0, len(values), 2)]
        total = values[0]
        strength[...] = total
        everything.wait_send()
    else:
        total = reduce(row_count, my_row, lambda d: (d, my_col), part, red_row, send_r, recv_r)
        part2 = red_col.at[col_count]
        part2[...] = total
        total = reduce(col_count, my_col, lambda d: (my_row, d), part2, red_col, send_r.at[pl.ds(row_count, col_count)], recv_r.at[pl.ds(row_count, col_count)])
        strength[...] = total
        close_last()
        finish_sends()


def closing(pixels, linked_in, comp_in, total, linked, comp, strength, scalars, sems):
    copies = [
        pltpu.make_async_copy(linked_in, linked, sems.at[0]),
        pltpu.make_async_copy(comp_in, comp, sems.at[1]),
        pltpu.make_async_copy(scalars, strength, sems.at[2]),
    ]
    for copy in copies[:2]:
        copy.start()
    for m in range(MS):
        scalars[m] = jnp.sum(total[m : m + 1]) / pixels
    copies[2].start()
    for copy in copies:
        copy.wait()


def shards(slc_stack, land_mask):
    rows, cols = land_mask.shape
    row_count, col_count = lax.axis_size("row"), lax.axis_size("col")
    f32, bf16 = jnp.float32, jnp.bfloat16
    vmem = pl.BlockSpec(memory_space=pltpu.VMEM)
    dma = pltpu.SemaphoreType.DMA
    hbm = pl.BlockSpec(memory_space=pltpu.HBM)
    devices = row_count * col_count
    direct = devices <= 64 and row_count & (row_count - 1) == 0 and col_count & (col_count - 1) == 0
    peers = devices if direct else row_count
    linked_shape = jax.ShapeDtypeStruct(slc_stack.shape, f32)
    comp_shape = jax.ShapeDtypeStruct((2, rows, cols), f32)
    linked, comp, total = pl.pallas_call(
        functools.partial(kernel, row_count, col_count, direct),
        out_shape=(linked_shape, comp_shape, jax.ShapeDtypeStruct((MS, cols), f32)),
        in_specs=[hbm, hbm],
        out_specs=(vmem, vmem, vmem),
        scratch_shapes=[
            pltpu.VMEM(slc_stack.shape, f32),
            pltpu.VMEM((rows, cols), jnp.int32),
            pltpu.VMEM((MS, rows * LINE + SUB, cols), f32),
            pltpu.VMEM((MS, EDGE + SUB, cols), f32),
            pltpu.VMEM((MS, EDGE + SUB, cols), f32),
            pltpu.VMEM((MS, 2, SUB, cols), f32),
            pltpu.VMEM((MS, 6, SUB, cols), f32),
            pltpu.VMEM((MS, 2, PACK, cols), f32),
            pltpu.VMEM((2 * rows, cols), f32),
            pltpu.VMEM((2 * rows, cols), f32),
            pltpu.VMEM((2 * rows, cols), f32),
            pltpu.VMEM((2, 2, cols), f32),
            pltpu.VMEM((6, 2, cols), f32),
            pltpu.VMEM((2, 2, cols), f32),
            pltpu.VMEM((2 * cols, cols), bf16),
            pltpu.VMEM((2 * cols, rows * cols), bf16),
            pltpu.VMEM((len(GROUPS) * rows * 2 * SUB, cols), f32),
            pltpu.VMEM((len(GROUPS), rows * 2 * SUB, 2 * cols), bf16),
            pltpu.VMEM((2 * FRESH_ROWS, 2 * cols), bf16),
            pltpu.VMEM((rows, FRESH_ROWS, cols), f32),
            pltpu.VMEM((rows * FRESH_STEP, cols), f32),
            pltpu.VMEM((rows * LATE_STEP, cols), f32),
            pltpu.VMEM((SLOTS, rows, cols), f32),
            pltpu.VMEM((MS, cols), f32),
            pltpu.VMEM((peers, MS, cols), f32),
            pltpu.VMEM((col_count + 1, MS, cols), f32),
            dma((MS + 1,)),
            pltpu.SemaphoreType.REGULAR((max(1, len(waves(row_count, col_count))),)),
            dma((len(AROUND),)),
            dma((MS, len(AROUND))),
            dma((len(AROUND),)),
            dma((len(AROUND),)),
            dma((1 if direct else row_count + col_count,)),
            dma((1 if direct else row_count + col_count,)),
        ],
        compiler_params=pltpu.CompilerParams(collective_id=0, has_side_effects=True, vmem_limit_bytes=16 << 20),
        name="linker",
    )(*(pltpu.with_memory_space_constraint(x, pltpu.HBM) for x in (slc_stack, land_mask)))
    return pl.pallas_call(
        functools.partial(closing, rows * cols * devices),
        out_shape=(linked_shape, comp_shape, jax.ShapeDtypeStruct((MS,), f32)),
        in_specs=[vmem, vmem, vmem],
        out_specs=(hbm, hbm, hbm),
        scratch_shapes=[pltpu.SMEM((MS,), f32), dma((3,))],
        compiler_params=pltpu.CompilerParams(vmem_limit_bytes=4 << 20),
        name="closing",
    )(linked, comp, total)


def solution(mesh):
    return jax.shard_map(
        shards,
        mesh=mesh,
        in_specs=(P(None, None, "row", "col"), P("row", "col")),
        out_specs=(P(None, None, "row", "col"), P(None, "row", "col"), P()),
        check_vma=False,
    )
```

```python
import functools

import jax
import jax.numpy as jnp
from jax import lax
from jax.experimental import pallas as pl
from jax.experimental.pallas import tpu as pltpu
from jax.sharding import PartitionSpec as P

M = 10
MS = 2
WIN = 11
ITERS = 4
REACH = WIN // 2
SUB = 8

covariance_floor = 8.0

AROUND = ((-1, 0), (1, 0), (-1, -1), (0, -1), (1, -1), (-1, 1), (0, 1), (1, 1))
LINE = 2 * M
EDGE = -(-REACH * LINE // SUB) * SUB
SKIP = EDGE - REACH * LINE
PACK = -(-LINE // SUB) * SUB


def pair_groups():
    groups = [[(s, (s + lag) % SUB) for s in range(SUB)] for lag in range(SUB // 2)]
    half = SUB // 2
    groups.insert(1, [(s, s + half) for s in range(half)] + [(M - 2, M - 1), (M - 2, M - 2), (M - 1, M - 1)])
    groups.append([(s, M - 2) for s in range(SUB)])
    groups.append([(s, M - 1) for s in range(SUB)])
    return groups


def field_rows(groups):
    table = {}
    for unit, group in enumerate(groups):
        for lane, (i, j) in enumerate(group):
            for part in range(1 if i == j else 2):
                table[(i, j, part)] = unit * 2 * SUB + part * SUB + lane
    return table


GROUPS = pair_groups()
LATE = [[(s, M) for s in range(SUB)], [(M, M)] * (2 * SUB - M) + [(s, M) for s in range(SUB, M)]]
FIELDS = field_rows(GROUPS)
LATE_FIELDS = field_rows(LATE)
PAIRS = [(i, j) for i, j, part in FIELDS if part == 1]
LATE_PAIRS = [(i, j) for i, j, part in LATE_FIELDS if part == 1]
FRESH_ROWS = len(GROUPS) * 2 * SUB
LATE_ROWS = len(LATE) * 2 * SUB
FRESH_STEP = FRESH_ROWS + 4
LATE_STEP = LATE_ROWS + 4
SLOTS = 3 * (len(PAIRS) + len(LATE_PAIRS)) + M + 1


def own_range(r, rows):
    return max(r, REACH), min(r + WIN, REACH + rows)


def own_sums(lines, rows):
    core = lines[rows - 1 - REACH]
    for e in range(rows, WIN):
        core = core + lines[e - REACH]
    starts = {rows - 1: core}
    for e in range(rows - 2, REACH - 1, -1):
        starts[e] = starts[e + 1] + lines[e - REACH]
    tails = {WIN: None}
    for e in range(WIN, REACH + rows):
        tails[e + 1] = lines[e - REACH] if tails[e] is None else tails[e] + lines[e - REACH]
    sums = {}
    for r in range(rows):
        start, stop = own_range(r, rows)
        if (start, stop) not in sums:
            tail = tails[stop]
            sums[(start, stop)] = starts[start] if tail is None else starts[start] + tail
    return sums


def window_sums(above, below, partial, rows):
    lead = {REACH: None}
    for e in range(REACH - 1, -1, -1):
        lead[e] = above[e] if lead[e + 1] is None else lead[e + 1] + above[e]
    trail = {0: None}
    for e in range(REACH):
        trail[e + 1] = below[e] if trail[e] is None else trail[e] + below[e]
    sums = []
    for r in range(rows):
        total = partial(r)
        for extra in (lead[min(r, REACH)], trail[max(0, r + WIN - REACH - rows)]):
            if extra is not None:
                total = total + extra
        sums.append(total)
    return sums


def split(value):
    high = value.astype(jnp.bfloat16)
    low = (value - high.astype(jnp.float32)).astype(jnp.bfloat16)
    return high, low


def waves(row_count, col_count):
    offsets = []
    known = 1
    while known < max(row_count, col_count) - 1:
        offsets.append(known)
        known *= 2
    return offsets


def kernel(
    row_count,
    col_count,
    direct,
    slc_hbm,
    land_hbm,
    linked,
    comp_out,
    strength,
    slc,
    land,
    own,
    up,
    dn,
    pack_send,
    pack_recv,
    halo,
    comp_send,
    comp_up,
    comp_dn,
    cpack_send,
    cpack_recv,
    chalo,
    w_main,
    w_halo,
    pbuf,
    ybuf,
    hbuf,
    ebuf,
    zbuf,
    zcbuf,
    coh,
    part,
    red_row,
    red_col,
    load_sem,
    ready,
    send_a,
    recv_a,
    send_b,
    recv_b,
    send_r,
    recv_r,
):
    rows, cols = land.shape
    my_row = lax.axis_index("row")
    my_col = lax.axis_index("col")
    strip = rows * REACH
    mesh_id = pl.DeviceIdType.MESH
    loads = [
        pltpu.make_async_copy(land_hbm, land, load_sem.at[MS]),
    ] + [
        pltpu.make_async_copy(slc_hbm.at[pl.ds(m * M, M)], slc.at[pl.ds(m * M, M)], load_sem.at[m]) for m in range(MS)
    ]
    for load in loads:
        load.start()

    def existing(dr, dc, far=1):
        ok = None
        for pos, step, count in ((my_row, dr, row_count), (my_col, dc, col_count)):
            if step:
                here = (pos >= far) if step < 0 else (pos < count - far)
                ok = here if ok is None else jnp.logical_and(ok, here)
        return ok

    exists = [existing(dr, dc) for dr, dc in AROUND]

    def greet(semaphore, far):
        expected = jnp.int32(0)
        for dr, dc in sorted(AROUND, key=lambda step: -abs(step[0]) - abs(step[1])):
            if (dr and far >= row_count) or (dc and far >= col_count):
                continue
            there = existing(dr, dc, far)

            @pl.when(there)
            def _(dr=dr, dc=dc):
                pl.semaphore_signal(
                    semaphore,
                    inc=1,
                    device_id=(my_row + dr * far, my_col + dc * far),
                    device_id_type=mesh_id,
                )

            expected = expected + there.astype(jnp.int32)
        return expected

    barrier = pltpu.get_barrier_semaphore()
    expected = greet(barrier, 1)
    offsets = waves(row_count, col_count)
    pending = []

    def next_wave():
        if pending:
            index, count = pending.pop()
            pl.semaphore_wait(ready.at[index], count)
            index += 1
        else:
            index = 0
        if index < len(offsets):
            pending.append((index, greet(ready.at[index], offsets[index])))

    for k, (dr, dc) in enumerate(AROUND):

        @pl.when(jnp.logical_not(exists[k]))
        def _(k=k, dc=dc, dr=dr):
            if dc == 0:
                target, small = (up, comp_up) if dr < 0 else (dn, comp_dn)
                for m in range(MS):
                    target[m] = jnp.zeros(target.shape[1:], jnp.float32)
                small[...] = jnp.zeros_like(small)
            else:
                for m in range(MS):
                    pack_recv[m, k - 2] = jnp.zeros(pack_recv.shape[2:], jnp.float32)
                cpack_recv[k - 2] = jnp.zeros(cpack_recv.shape[1:], jnp.float32)

    lane = lax.broadcasted_iota(jnp.int32, (rows, cols), 1)
    sub = lax.broadcasted_iota(jnp.int32, (rows, cols), 0)

    for load in loads[:2]:
        load.wait()
    mask = land[...].astype(jnp.float32)

    def place(m):
        for i in range(M):
            for c in range(2):
                own[m, pl.ds(c * M + i, rows, stride=LINE), :] = slc[m * M + i, c] * mask
        own[m, rows * LINE :, :] = jnp.zeros((own.shape[1] - rows * LINE, cols), jnp.float32)

    def pack(m):
        packed = [jnp.zeros((SUB, cols), jnp.float32)] * 2
        for block in range(PACK // SUB):
            at = block * SUB
            low = high = jnp.zeros((SUB, cols), jnp.float32)
            for r in range(rows):
                turned = pltpu.roll(own[m, r * LINE + at : r * LINE + at + SUB, :], REACH * (r + 1), 1)
                high = jnp.where((lane >= r * REACH) & (lane < (r + 1) * REACH), turned, high)
                low = jnp.where((lane >= (r + 1) * REACH) & (lane < (r + 2) * REACH), turned, low)
            here = (lane >= block * strip) & (lane < (block + 1) * strip)
            for side, value in enumerate((pltpu.roll(low, (block * strip - REACH) % cols, 1), high)):
                if side and block:
                    value = pltpu.roll(value, block * strip, 1)
                packed[side] = jnp.where(here, value, packed[side])
        for side in range(2):
            pack_send[m, side] = packed[side]

    def mirror(k):
        dr, dc = AROUND[k]
        return AROUND.index((-dr, -dc))

    def fresh_pair(m, k, sending):
        dr, dc = AROUND[k]
        back = mirror(k)
        slot = back if sending else k
        if dc == 0:
            source = own.at[m, pl.ds(0 if dr < 0 else rows * LINE - EDGE, EDGE)]
            target = (up if AROUND[slot][0] < 0 else dn).at[m, pl.ds(0, EDGE)]
        else:
            source = pack_send.at[m, 0 if dc < 0 else 1]
            target = pack_recv.at[m, slot - 2]
        return pltpu.make_async_remote_copy(
            src_ref=source,
            dst_ref=target,
            send_sem=send_a.at[k],
            recv_sem=recv_a.at[m, slot],
            device_id=(my_row + dr, my_col + dc),
            device_id_type=mesh_id,
        )

    def each_around(action, which=range(len(AROUND))):
        for k in which:

            @pl.when(exists[k])
            def _(k=k):
                action(k)

    beside, strips = range(2), range(2, len(AROUND))
    outward = (2, 4, 5, 7, 3, 6, 0, 1)
    place(0)
    pack(0)
    pl.semaphore_wait(barrier, expected)
    each_around(lambda k: fresh_pair(0, k, True).start(), outward)
    next_wave()

    k_at = lax.broadcasted_iota(jnp.int32, (cols, cols), 0)
    n_at = lax.broadcasted_iota(jnp.int32, (cols, cols), 1)
    near = jnp.where((k_at - n_at <= REACH) & (n_at - k_at <= REACH), 1.0, 0.0).astype(jnp.bfloat16)
    w_main[0:cols, :] = near
    w_main[cols:, :] = near
    line_of = k_at // REACH
    inner = k_at - line_of * REACH
    for side in range(2):
        touches = (n_at <= inner) if side == 0 else (n_at >= inner + cols - REACH)
        line = jnp.where(touches, line_of, -1)
        for r in range(rows):
            first = rows - REACH + r
            w_halo[side * cols : (side + 1) * cols, r * cols : (r + 1) * cols] = jnp.where(
                (line >= first) & (line < first + WIN), 1.0, 0.0
            ).astype(jnp.bfloat16)

    lines_total = WIN + rows - 1

    def gather_halo(parts):
        sides = []
        for side in range(2):
            a, b, c = (parts(side * 3 + j) for j in range(3))
            which = lax.broadcasted_iota(jnp.int32, a.shape, 1)
            sides.append(jnp.where(which < strip, a, jnp.where(which < 2 * strip, b, c)))
        return sides

    def line_tile(m, e, c, first):
        if e < REACH:
            buffer, at = up, SKIP + e * LINE
        elif e < REACH + rows:
            buffer, at = own, (e - REACH) * LINE
        else:
            buffer, at = dn, (e - REACH - rows) * LINE
        at += c * M + first
        return buffer[m, at : at + SUB, :]

    def halo_tile(m, side, c, first):
        at = c * M + first
        return halo[m, side, at : at + SUB, :]

    def real_part(a, b, x, y):
        return a * x + b * y

    def imag_part(a, b, x, y):
        return b * x - a * y

    def operands(tile, unit):
        lead = [tile(c, 0) for c in range(2)]
        if unit == 0:
            return lead, lead
        if 1 < unit <= SUB // 2:
            return lead, [pltpu.roll(v, SUB + 1 - unit, 0) for v in lead]
        if unit == 1:
            left, right = [], []
            for c in range(2):
                mid, late = tile(c, SUB // 2), tile(c, SUB - M + 5)
                left.append(jnp.where(sub < 4, lead[c], jnp.where(sub == 4, mid, late)))
                right.append(jnp.where(sub < 4, mid, jnp.where(sub == 4, tile(c, 5), late)))
            return left, right
        return lead, None

    def products(tile, row_tile, unit):
        (a, b), other = operands(tile, unit)
        if unit == 0:
            return a * a + b * b, None
        if other is None:
            image = M - 3 + unit - SUB // 2
            x, y = (jnp.broadcast_to(row_tile(c, image), (SUB, cols)) for c in range(2))
        else:
            x, y = other
        return real_part(a, b, x, y), imag_part(a, b, x, y)

    def tile_of(m, e):
        if e < lines_total:
            return functools.partial(line_tile, m, e)
        return functools.partial(halo_tile, m, e - lines_total)

    def row_of(m, e):
        tile = tile_of(m, e)
        return lambda c, image: tile(c, image)[0:1]

    def emit_side(unit, side, value, count):
        high, low = split(value)
        at = unit * 2 * SUB
        hbuf[at : at + 2 * SUB, side * cols : (side + 1) * cols] = high
        hbuf[count + at : count + at + 2 * SUB, side * cols : (side + 1) * cols] = low

    def edges(count):
        for r in range(0, rows, 2):
            band = w_halo[:, r * cols : (r + 2) * cols]
            value = jnp.dot(hbuf[0 : 2 * count], band, preferred_element_type=jnp.float32)
            value = value[0:count] + value[count:]
            ebuf[r, 0:count] = value[:, 0:cols]
            ebuf[r + 1, 0:count] = value[:, cols:]

    partials = {}
    for r in range(rows):
        partials.setdefault(own_range(r, rows), len(partials))

    def keep_own(unit, lines):
        for key, value in own_sums(lines, rows).items():
            at = (unit * len(partials) + partials[key]) * 2 * SUB
            pbuf[at : at + 2 * SUB, :] = value

    def emit_lines(unit, lines):
        def partial(r):
            at = (unit * len(partials) + partials[own_range(r, rows)]) * 2 * SUB
            return pbuf[at : at + 2 * SUB, :]

        for r, total in enumerate(window_sums(lines[:REACH], lines[REACH:], partial, rows)):
            high, low = split(total)
            ybuf[unit, r * 2 * SUB : (r + 1) * 2 * SUB, 0:cols] = high
            ybuf[unit, r * 2 * SUB : (r + 1) * 2 * SUB, cols:] = low

    def emit_main(unit, main, target, step):
        for r in range(rows):
            at = r * step + unit * 2 * SUB
            target[at : at + 2 * SUB, :] = (
                main[r * 2 * SUB : (r + 1) * 2 * SUB, :] + ebuf[r, unit * 2 * SUB : (unit + 1) * 2 * SUB]
            )

    def both_halves(pair):
        first, second = pair
        return jnp.concatenate([first, jnp.zeros_like(first) if second is None else second], 0)

    own_lines = range(REACH, REACH + rows)
    far_lines = [*range(REACH), *range(REACH + rows, lines_total)]

    def fresh_values(m, e, unit):
        return both_halves(products(tile_of(m, e), row_of(m, e), unit))

    def fresh_own(m):
        for unit in range(len(GROUPS)):
            keep_own(unit, [fresh_values(m, e, unit) for e in own_lines])

    def fresh_sides(m):
        for side in range(2):
            for unit in range(len(GROUPS)):
                emit_side(unit, side, fresh_values(m, lines_total + side, unit), FRESH_ROWS)
        edges(FRESH_ROWS)

    def fresh_far(m):
        for unit in range(len(GROUPS)):
            emit_lines(unit, [fresh_values(m, e, unit) for e in far_lines])
            main = jnp.dot(ybuf[unit], w_main[...], preferred_element_type=jnp.float32)
            emit_main(unit, main, zbuf, FRESH_STEP)

    def comp_row(e, c):
        if e < REACH:
            at = c * rows + rows - REACH + e
            return comp_up[at : at + 1, :]
        if e < REACH + rows:
            at = c * rows + e - REACH
            return comp_send[at : at + 1, :]
        if e < lines_total:
            at = c * rows + e - REACH - rows
            return comp_dn[at : at + 1, :]
        return chalo[e - lines_total, c : c + 1, :]

    def late_products(m, e, unit):
        tile = tile_of(m, e)
        x, y = (jnp.broadcast_to(comp_row(e, c), (SUB, cols)) for c in range(2))
        if unit == 0:
            a, b = tile(0, 0), tile(1, 0)
        else:
            a, b = (jnp.where(sub < 2 * SUB - M, v, tile(c, M - SUB)) for c, v in enumerate((x, y)))
        return jnp.concatenate([real_part(a, b, x, y), imag_part(a, b, x, y)], 0)

    def late_fields(m):
        for side in range(2):
            for unit in range(len(LATE)):
                emit_side(unit, side, late_products(m, lines_total + side, unit), LATE_ROWS)
        edges(LATE_ROWS)
        for unit in range(len(LATE)):
            emit_lines(unit, [late_products(m, e, unit) for e in far_lines])
        size = rows * 2 * SUB
        main = jnp.dot(
            ybuf[0 : len(LATE)].reshape(len(LATE) * size, 2 * cols), w_main[...], preferred_element_type=jnp.float32
        )
        for unit in range(len(LATE)):
            emit_main(unit, main[unit * size : (unit + 1) * size], zcbuf, LATE_STEP)

    def late_own(m):
        for unit in range(len(LATE)):
            keep_own(unit, [late_products(m, e, unit) for e in own_lines])

    def fresh_field(i, j, p):
        return zbuf[pl.ds(FIELDS[(i, j, p)], rows, stride=FRESH_STEP), :]

    def late_field(i, j, p):
        return zcbuf[pl.ds(LATE_FIELDS[(i, j, p)], rows, stride=LATE_STEP), :]

    class Coherence:
        def __init__(self):
            self.scales = {}
            self.slot = {}
            self.re = {}
            self.im = {}
            self.used = 0

        def keep(self, key, value):
            coh[self.used] = value
            self.slot[key] = self.used
            self.used += 1

        def get(self, key):
            return coh[self.slot[key]]

        def tally(self, sums, i, value, minus=False):
            if i in sums:
                sums[i] = sums[i] - value if minus else sums[i] + value
            else:
                sums[i] = -value if minus else value

        def add(self, images, pairs, field):
            for i in images:
                value = field(i, i, 0)
                scale = lax.rsqrt(jnp.maximum(value, covariance_floor))
                self.scales[i] = scale
                value = value * (scale * scale)
                self.keep((i, i), value)
                self.tally(self.re, i, value)
            for i, j in pairs:
                s = self.scales[i] * self.scales[j]
                c = field(i, j, 0) * s
                d = field(i, j, 1) * s
                self.keep((i, j, 0), c)
                self.keep((i, j, 1), c + d)
                self.keep((i, j, 2), c - d)
                self.tally(self.re, i, c)
                self.tally(self.re, j, c)
                self.tally(self.im, i, d)
                self.tally(self.im, j, d, True)

        def power(self):
            images = sorted(self.re)
            re = [self.re[i] for i in images]
            im = [self.im[i] for i in images]
            gain = None
            for step in range(ITERS):
                if step:
                    both = [x + y for x, y in zip(re, im)]
                    new_re, new_im = [], []
                    for i in images:
                        shared = first = second = None
                        for j in images:
                            if j == i:
                                continue
                            key = (i, j) if (i, j, 0) in self.slot else (j, i)
                            turn = key != (i, j)
                            c = self.get(key + (0,)) * both[j]
                            e = self.get(key + (2 if turn else 1,)) * im[j]
                            f = self.get(key + (1 if turn else 2,)) * re[j]
                            shared = c if shared is None else shared + c
                            first = e if first is None else first + e
                            second = f if second is None else second + f
                        c = self.get((i, i))
                        new_re.append((shared - first) + c * re[i])
                        new_im.append((shared - second) + c * im[i])
                    re, im = new_re, new_im
                squares = [x * x + y * y for x, y in zip(re, im)]
                while len(squares) > 1:
                    squares = [sum(squares[k + 1 : k + 2], squares[k]) for k in range(0, len(squares), 2)]
                square = squares[0] if gain is None else squares[0] * (gain * gain)
                inverse = lax.rsqrt(jnp.maximum(square, 1.0))
                gain = inverse if gain is None else gain * inverse
            return jnp.sqrt(square), gain, re, im

    def finish(m, number, length, gain, re, im):
        comp_re = comp_im = None
        for i in range(M):
            a = own[m, pl.ds(i, rows, stride=LINE), :]
            b = own[m, pl.ds(M + i, rows, stride=LINE), :]
            x = re[i] * a + im[i] * b
            y = re[i] * b - im[i] * a
            comp_re = x if comp_re is None else comp_re + x
            comp_im = y if comp_im is None else comp_im + y
        return comp_re * gain, comp_im * gain

    def put_linked(m, gain, re, im):
        factor = gain * mask
        for i in range(M):
            linked[m * M + i, 0] = re[i] * factor
            linked[m * M + i, 1] = im[i] * factor

    def share_of(number, length):
        return jnp.sum(mask * length, axis=0, keepdims=True) * (1.0 / number)

    def take_strips(m):
        each_around(lambda k: fresh_pair(m, k, False).wait_recv(), strips)
        for block in range(PACK // SUB):

            def turned(j, block=block):
                value = pack_recv[m, j]
                shift = (j % 3 - block) * strip % cols
                return pltpu.roll(value, shift, 1) if shift else value

            for side, value in enumerate(gather_halo(turned)):
                halo[m, side, block * SUB : (block + 1) * SUB, :] = value

    def take_beside(m):
        each_around(lambda k: fresh_pair(m, k, False).wait_recv(), beside)

    fresh_own(0)
    for m in range(1, MS):
        loads[1 + m].wait()
        place(m)
        pack(m)
    take_strips(0)
    for m in range(1, MS):
        each_around(lambda k, m=m: fresh_pair(m, k, True).start(), outward)
    fresh_sides(0)
    next_wave()
    take_beside(0)
    fresh_far(0)
    early = Coherence()
    early.add(range(M), PAIRS, fresh_field)
    length, gain, re, im = early.power()
    comp_re, comp_im = finish(0, M, length, gain, re, im)
    comp_send[0:rows, :] = comp_re
    comp_send[rows:, :] = comp_im

    def comp_pair(k, sending):
        dr, dc = AROUND[k]
        slot = mirror(k) if sending else k
        if dc == 0:
            source = comp_send
            target = comp_up if AROUND[slot][0] < 0 else comp_dn
        else:
            source = cpack_send.at[0 if dc < 0 else 1]
            target = cpack_recv.at[slot - 2]
        return pltpu.make_async_remote_copy(
            src_ref=source,
            dst_ref=target,
            send_sem=send_b.at[k],
            recv_sem=recv_b.at[slot],
            device_id=(my_row + dr, my_col + dc),
            device_id_type=mesh_id,
        )

    each_around(lambda k: comp_pair(k, True).start(), beside)
    for c, value in enumerate((comp_re, comp_im)):
        for side in range(2):
            total = jnp.zeros((rows, cols), jnp.float32)
            for copy in range(3):
                turned = pltpu.roll(value, REACH * side + strip * copy, 1, stride=REACH, stride_axis=0)
                first = strip * copy + sub * REACH
                total = jnp.where((lane >= first) & (lane < first + REACH), turned, total)
            cpack_send[side, c : c + 1, :] = jnp.sum(total, axis=0, keepdims=True)

    each_around(lambda k: comp_pair(k, True).start(), (2, 4, 5, 7, 3, 6))

    put_linked(0, gain, re, im)
    part[0:1] = share_of(M, length)
    last = MS - 1
    fresh_own(last)
    take_strips(last)
    fresh_sides(last)
    take_beside(last)
    fresh_far(last)
    late_own(last)
    joint = Coherence()
    joint.add(range(M), PAIRS, fresh_field)
    while len(pending) and pending[0][0] < len(offsets) - 1:
        next_wave()

    each_around(lambda k: comp_pair(k, False).wait_recv())
    for side, value in enumerate(gather_halo(lambda j: cpack_recv[j])):
        chalo[side] = value
    late_fields(last)
    joint.add([M], LATE_PAIRS, late_field)
    length, gain, re, im = joint.power()
    part[last : last + 1] = share_of(M + 1, length)
    while pending:
        next_wave()

    def reduce(count, me, device, source, buffer, sends, recvs):
        copies = []
        for step in range(1, count):
            copy = pltpu.make_async_remote_copy(
                src_ref=source,
                dst_ref=buffer.at[me],
                send_sem=sends.at[step],
                recv_sem=recvs.at[me],
                device_id=device(lax.rem(me + step, count)),
                device_id_type=mesh_id,
            )
            copy.start()
            copies.append(copy)
        buffer[me] = source[...]
        for step in range(1, count):
            other = lax.rem(me + step, count)
            pltpu.make_async_remote_copy(
                src_ref=source,
                dst_ref=buffer.at[other],
                send_sem=sends.at[step],
                recv_sem=recvs.at[other],
                device_id=device(other),
                device_id_type=mesh_id,
            ).wait_recv()
        for copy in copies:
            copy.wait_send()
        total = buffer[0]
        for other in range(1, count):
            total = total + buffer[other]
        return total

    def close_last():
        comp_re, comp_im = finish(last, M + 1, length, gain, re, im)
        comp_out[0] = comp_re
        comp_out[1] = comp_im
        put_linked(last, gain, re, im)

    def sent(k):
        dr, dc = AROUND[k]
        if dc == 0:
            source, target = own.at[:, pl.ds(0, EDGE)], up.at[:, pl.ds(0, EDGE)]
        else:
            source, target = pack_send.at[:, 0], pack_recv.at[:, 0]
        return pltpu.make_async_remote_copy(
            src_ref=source,
            dst_ref=target,
            send_sem=send_a.at[k],
            recv_sem=recv_a.at[0, k],
            device_id=(my_row + dr, my_col + dc),
            device_id_type=mesh_id,
        )

    def finish_sends():
        each_around(lambda k: sent(k).wait_send())
        each_around(lambda k: comp_pair(k, True).wait_send())

    def flips(position, count):
        steps = []
        size = 1
        while size < count:
            steps.append(size * (1 - 2 * lax.rem(position // size, 2)))
            size *= 2
        return steps

    def swapped(position, steps, mask_bits):
        for bit, step in enumerate(steps):
            if mask_bits >> bit & 1:
                position = position + step
        return position

    if direct:
        count = row_count * col_count
        row_steps, col_steps = flips(my_row, row_count), flips(my_col, col_count)

        def weight(code):
            return -bin(code // col_count).count("1") - code % col_count

        for code in sorted(range(1, count), key=weight):
            pltpu.make_async_remote_copy(
                src_ref=part,
                dst_ref=red_row.at[code],
                send_sem=send_r.at[0],
                recv_sem=recv_r.at[0],
                device_id=(
                    swapped(my_row, row_steps, code // col_count),
                    swapped(my_col, col_steps, code % col_count),
                ),
                device_id_type=mesh_id,
            ).start()
        close_last()
        finish_sends()
        everything = pltpu.make_async_remote_copy(
            src_ref=red_row.at[pl.ds(1, count - 1)],
            dst_ref=red_row.at[pl.ds(1, count - 1)],
            send_sem=send_r.at[0],
            recv_sem=recv_r.at[0],
            device_id=(swapped(my_row, row_steps, row_count - 1), swapped(my_col, col_steps, col_count - 1)),
            device_id_type=mesh_id,
        )
        everything.wait_recv()
        values = [part[...]] + [red_row[code] for code in range(1, count)]
        while len(values) > 1:
            values = [values[k] + values[k + 1] for k in range(0, len(values), 2)]
        total = values[0]
        strength[...] = total
        everything.wait_send()
    else:
        total = reduce(row_count, my_row, lambda d: (d, my_col), part, red_row, send_r, recv_r)
        part2 = red_col.at[col_count]
        part2[...] = total
        total = reduce(col_count, my_col, lambda d: (my_row, d), part2, red_col, send_r.at[pl.ds(row_count, col_count)], recv_r.at[pl.ds(row_count, col_count)])
        strength[...] = total
        close_last()
        finish_sends()


def closing(pixels, linked_in, comp_in, total, linked, comp, strength, scalars, sems):
    copies = [
        pltpu.make_async_copy(linked_in, linked, sems.at[0]),
        pltpu.make_async_copy(comp_in, comp, sems.at[1]),
        pltpu.make_async_copy(scalars, strength, sems.at[2]),
    ]
    for copy in copies[:2]:
        copy.start()
    sums = jnp.sum(total[...], axis=1, keepdims=True) * (1.0 / pixels)
    for m in range(MS):
        scalars[m] = sums[m, 0]
    copies[2].start()
    for copy in copies:
        copy.wait()


def shards(slc_stack, land_mask):
    rows, cols = land_mask.shape
    row_count, col_count = lax.axis_size("row"), lax.axis_size("col")
    f32, bf16 = jnp.float32, jnp.bfloat16
    vmem = pl.BlockSpec(memory_space=pltpu.VMEM)
    dma = pltpu.SemaphoreType.DMA
    hbm = pl.BlockSpec(memory_space=pltpu.HBM)
    devices = row_count * col_count
    direct = devices <= 64 and row_count & (row_count - 1) == 0 and col_count & (col_count - 1) == 0
    peers = devices if direct else row_count
    linked_shape = jax.ShapeDtypeStruct(slc_stack.shape, f32)
    comp_shape = jax.ShapeDtypeStruct((2, rows, cols), f32)
    linked, comp, total = pl.pallas_call(
        functools.partial(kernel, row_count, col_count, direct),
        out_shape=(linked_shape, comp_shape, jax.ShapeDtypeStruct((MS, cols), f32)),
        in_specs=[hbm, hbm],
        out_specs=(vmem, vmem, vmem),
        scratch_shapes=[
            pltpu.VMEM(slc_stack.shape, f32),
            pltpu.VMEM((rows, cols), jnp.int32),
            pltpu.VMEM((MS, rows * LINE + SUB, cols), f32),
            pltpu.VMEM((MS, EDGE + SUB, cols), f32),
            pltpu.VMEM((MS, EDGE + SUB, cols), f32),
            pltpu.VMEM((MS, 2, SUB, cols), f32),
            pltpu.VMEM((MS, 6, SUB, cols), f32),
            pltpu.VMEM((MS, 2, PACK, cols), f32),
            pltpu.VMEM((2 * rows, cols), f32),
            pltpu.VMEM((2 * rows, cols), f32),
            pltpu.VMEM((2 * rows, cols), f32),
            pltpu.VMEM((2, 2, cols), f32),
            pltpu.VMEM((6, 2, cols), f32),
            pltpu.VMEM((2, 2, cols), f32),
            pltpu.VMEM((2 * cols, cols), bf16),
            pltpu.VMEM((2 * cols, rows * cols), bf16),
            pltpu.VMEM((len(GROUPS) * rows * 2 * SUB, cols), f32),
            pltpu.VMEM((len(GROUPS), rows * 2 * SUB, 2 * cols), bf16),
            pltpu.VMEM((2 * FRESH_ROWS, 2 * cols), bf16),
            pltpu.VMEM((rows, FRESH_ROWS, cols), f32),
            pltpu.VMEM((rows * FRESH_STEP, cols), f32),
            pltpu.VMEM((rows * LATE_STEP, cols), f32),
            pltpu.VMEM((SLOTS, rows, cols), f32),
            pltpu.VMEM((MS, cols), f32),
            pltpu.VMEM((peers, MS, cols), f32),
            pltpu.VMEM((col_count + 1, MS, cols), f32),
            dma((MS + 1,)),
            pltpu.SemaphoreType.REGULAR((max(1, len(waves(row_count, col_count))),)),
            dma((len(AROUND),)),
            dma((MS, len(AROUND))),
            dma((len(AROUND),)),
            dma((len(AROUND),)),
            dma((1 if direct else row_count + col_count,)),
            dma((1 if direct else row_count + col_count,)),
        ],
        compiler_params=pltpu.CompilerParams(collective_id=0, has_side_effects=True, vmem_limit_bytes=16 << 20),
        name="linker",
    )(*(pltpu.with_memory_space_constraint(x, pltpu.HBM) for x in (slc_stack, land_mask)))
    return pl.pallas_call(
        functools.partial(closing, rows * cols * devices),
        out_shape=(linked_shape, comp_shape, jax.ShapeDtypeStruct((MS,), f32)),
        in_specs=[vmem, vmem, vmem],
        out_specs=(hbm, hbm, hbm),
        scratch_shapes=[pltpu.SMEM((MS,), f32), dma((3,))],
        compiler_params=pltpu.CompilerParams(vmem_limit_bytes=4 << 20),
        name="closing",
    )(linked, comp, total)


def solution(mesh):
    return jax.shard_map(
        shards,
        mesh=mesh,
        in_specs=(P(None, None, "row", "col"), P("row", "col")),
        out_specs=(P(None, None, "row", "col"), P(None, "row", "col"), P()),
        check_vma=False,
    )
```

```python
import functools

import jax
import jax.numpy as jnp
from jax import lax
from jax.experimental import pallas as pl
from jax.experimental.pallas import tpu as pltpu
from jax.sharding import PartitionSpec as P

M = 10
MS = 2
WIN = 11
ITERS = 4
REACH = WIN // 2
SUB = 8

covariance_floor = 8.0

AROUND = ((-1, 0), (1, 0), (-1, -1), (0, -1), (1, -1), (-1, 1), (0, 1), (1, 1))
LINE = 2 * M
EDGE = -(-REACH * LINE // SUB) * SUB
SKIP = EDGE - REACH * LINE
PACK = -(-LINE // SUB) * SUB


def pair_groups():
    groups = [[(s, (s + lag) % SUB) for s in range(SUB)] for lag in range(SUB // 2)]
    half = SUB // 2
    groups.insert(1, [(s, s + half) for s in range(half)] + [(M - 2, M - 1), (M - 2, M - 2), (M - 1, M - 1)])
    groups.append([(s, M - 2) for s in range(SUB)])
    groups.append([(s, M - 1) for s in range(SUB)])
    return groups


def field_rows(groups):
    table = {}
    for unit, group in enumerate(groups):
        for lane, (i, j) in enumerate(group):
            for part in range(1 if i == j else 2):
                table[(i, j, part)] = unit * 2 * SUB + part * SUB + lane
    return table


GROUPS = pair_groups()
LATE = [[(s, M) for s in range(SUB)], [(M, M)] * (2 * SUB - M) + [(s, M) for s in range(SUB, M)]]
FIELDS = field_rows(GROUPS)
LATE_FIELDS = field_rows(LATE)
PAIRS = [(i, j) for i, j, part in FIELDS if part == 1]
LATE_PAIRS = [(i, j) for i, j, part in LATE_FIELDS if part == 1]
FRESH_ROWS = len(GROUPS) * 2 * SUB
LATE_ROWS = len(LATE) * 2 * SUB
FRESH_STEP = FRESH_ROWS + 4
LATE_STEP = LATE_ROWS + 4
SLOTS = 3 * (len(PAIRS) + len(LATE_PAIRS)) + M + 1


def own_range(r, rows):
    return max(r, REACH), min(r + WIN, REACH + rows)


def own_sums(lines, rows):
    core = lines[rows - 1 - REACH]
    for e in range(rows, WIN):
        core = core + lines[e - REACH]
    starts = {rows - 1: core}
    for e in range(rows - 2, REACH - 1, -1):
        starts[e] = starts[e + 1] + lines[e - REACH]
    tails = {WIN: None}
    for e in range(WIN, REACH + rows):
        tails[e + 1] = lines[e - REACH] if tails[e] is None else tails[e] + lines[e - REACH]
    sums = {}
    for r in range(rows):
        start, stop = own_range(r, rows)
        if (start, stop) not in sums:
            tail = tails[stop]
            sums[(start, stop)] = starts[start] if tail is None else starts[start] + tail
    return sums


def window_sums(above, below, partial, rows):
    lead = {REACH: None}
    for e in range(REACH - 1, -1, -1):
        lead[e] = above[e] if lead[e + 1] is None else lead[e + 1] + above[e]
    trail = {0: None}
    for e in range(REACH):
        trail[e + 1] = below[e] if trail[e] is None else trail[e] + below[e]
    sums = []
    for r in range(rows):
        total = partial(r)
        for extra in (lead[min(r, REACH)], trail[max(0, r + WIN - REACH - rows)]):
            if extra is not None:
                total = total + extra
        sums.append(total)
    return sums


def split(value):
    high = value.astype(jnp.bfloat16)
    low = (value - high.astype(jnp.float32)).astype(jnp.bfloat16)
    return high, low


def waves(row_count, col_count):
    offsets = []
    known = 1
    while known < max(row_count, col_count) - 1:
        offsets.append(known)
        known *= 2
    return offsets


def kernel(
    row_count,
    col_count,
    direct,
    slc_hbm,
    land_hbm,
    linked,
    comp_out,
    strength,
    slc,
    land,
    own,
    up,
    dn,
    pack_send,
    pack_recv,
    halo,
    comp_send,
    comp_up,
    comp_dn,
    cpack_send,
    cpack_recv,
    chalo,
    w_main,
    w_halo,
    pbuf,
    ybuf,
    hbuf,
    ebuf,
    zbuf,
    zcbuf,
    coh,
    part,
    red_row,
    red_col,
    load_sem,
    ready,
    send_a,
    recv_a,
    send_b,
    recv_b,
    send_r,
    recv_r,
):
    rows, cols = land.shape
    my_row = lax.axis_index("row")
    my_col = lax.axis_index("col")
    strip = rows * REACH
    mesh_id = pl.DeviceIdType.MESH
    loads = [
        pltpu.make_async_copy(land_hbm, land, load_sem.at[MS]),
    ] + [
        pltpu.make_async_copy(slc_hbm.at[pl.ds(m * M, M)], slc.at[pl.ds(m * M, M)], load_sem.at[m]) for m in range(MS)
    ]

    def existing(dr, dc, far=1):
        ok = None
        for pos, step, count in ((my_row, dr, row_count), (my_col, dc, col_count)):
            if step:
                here = (pos >= far) if step < 0 else (pos < count - far)
                ok = here if ok is None else jnp.logical_and(ok, here)
        return ok

    exists = [existing(dr, dc) for dr, dc in AROUND]

    def greet(semaphore, far):
        expected = jnp.int32(0)
        for dr, dc in sorted(AROUND, key=lambda step: -abs(step[0]) - abs(step[1])):
            if (dr and far >= row_count) or (dc and far >= col_count):
                continue
            there = existing(dr, dc, far)

            @pl.when(there)
            def _(dr=dr, dc=dc):
                pl.semaphore_signal(
                    semaphore,
                    inc=1,
                    device_id=(my_row + dr * far, my_col + dc * far),
                    device_id_type=mesh_id,
                )

            expected = expected + there.astype(jnp.int32)
        return expected

    barrier = pltpu.get_barrier_semaphore()
    expected = greet(barrier, 1)
    for load in loads:
        load.start()
    offsets = waves(row_count, col_count)
    pending = []

    def next_wave():
        if pending:
            index, count = pending.pop()
            pl.semaphore_wait(ready.at[index], count)
            index += 1
        else:
            index = 0
        if index < len(offsets):
            pending.append((index, greet(ready.at[index], offsets[index])))

    for k, (dr, dc) in enumerate(AROUND):

        @pl.when(jnp.logical_not(exists[k]))
        def _(k=k, dc=dc, dr=dr):
            if dc == 0:
                target, small = (up, comp_up) if dr < 0 else (dn, comp_dn)
                for m in range(MS):
                    target[m] = jnp.zeros(target.shape[1:], jnp.float32)
                small[...] = jnp.zeros_like(small)
            else:
                for m in range(MS):
                    pack_recv[m, k - 2] = jnp.zeros(pack_recv.shape[2:], jnp.float32)
                cpack_recv[k - 2] = jnp.zeros(cpack_recv.shape[1:], jnp.float32)

    lane = lax.broadcasted_iota(jnp.int32, (rows, cols), 1)
    sub = lax.broadcasted_iota(jnp.int32, (rows, cols), 0)

    for load in loads[:2]:
        load.wait()
    mask = land[...].astype(jnp.float32)

    def place(m):
        for i in range(M):
            for c in range(2):
                own[m, pl.ds(c * M + i, rows, stride=LINE), :] = slc[m * M + i, c] * mask
        own[m, rows * LINE :, :] = jnp.zeros((own.shape[1] - rows * LINE, cols), jnp.float32)

    def pack(m):
        packed = [jnp.zeros((SUB, cols), jnp.float32)] * 2
        for block in range(PACK // SUB):
            at = block * SUB
            low = high = jnp.zeros((SUB, cols), jnp.float32)
            for r in range(rows):
                turned = pltpu.roll(own[m, r * LINE + at : r * LINE + at + SUB, :], REACH * (r + 1), 1)
                high = jnp.where((lane >= r * REACH) & (lane < (r + 1) * REACH), turned, high)
                low = jnp.where((lane >= (r + 1) * REACH) & (lane < (r + 2) * REACH), turned, low)
            here = (lane >= block * strip) & (lane < (block + 1) * strip)
            for side, value in enumerate((pltpu.roll(low, (block * strip - REACH) % cols, 1), high)):
                if side and block:
                    value = pltpu.roll(value, block * strip, 1)
                packed[side] = jnp.where(here, value, packed[side])
        for side in range(2):
            pack_send[m, side] = packed[side]

    def mirror(k):
        dr, dc = AROUND[k]
        return AROUND.index((-dr, -dc))

    def fresh_pair(m, k, sending):
        dr, dc = AROUND[k]
        back = mirror(k)
        slot = back if sending else k
        if dc == 0:
            source = own.at[m, pl.ds(0 if dr < 0 else rows * LINE - EDGE, EDGE)]
            target = (up if AROUND[slot][0] < 0 else dn).at[m, pl.ds(0, EDGE)]
        else:
            source = pack_send.at[m, 0 if dc < 0 else 1]
            target = pack_recv.at[m, slot - 2]
        return pltpu.make_async_remote_copy(
            src_ref=source,
            dst_ref=target,
            send_sem=send_a.at[k],
            recv_sem=recv_a.at[m, slot],
            device_id=(my_row + dr, my_col + dc),
            device_id_type=mesh_id,
        )

    def each_around(action, which=range(len(AROUND))):
        for k in which:

            @pl.when(exists[k])
            def _(k=k):
                action(k)

    beside, strips = range(2), range(2, len(AROUND))
    outward = (2, 4, 5, 7, 3, 6, 0, 1)
    place(0)
    pack(0)
    pl.semaphore_wait(barrier, expected)
    each_around(lambda k: fresh_pair(0, k, True).start(), outward)
    next_wave()

    k_at = lax.broadcasted_iota(jnp.int32, (cols, cols), 0)
    n_at = lax.broadcasted_iota(jnp.int32, (cols, cols), 1)
    near = jnp.where((k_at - n_at <= REACH) & (n_at - k_at <= REACH), 1.0, 0.0).astype(jnp.bfloat16)
    w_main[0:cols, :] = near
    w_main[cols:, :] = near
    line_of = k_at // REACH
    inner = k_at - line_of * REACH
    for side in range(2):
        touches = (n_at <= inner) if side == 0 else (n_at >= inner + cols - REACH)
        line = jnp.where(touches, line_of, -1)
        for r in range(rows):
            first = rows - REACH + r
            w_halo[side * cols : (side + 1) * cols, r * cols : (r + 1) * cols] = jnp.where(
                (line >= first) & (line < first + WIN), 1.0, 0.0
            ).astype(jnp.bfloat16)

    lines_total = WIN + rows - 1

    def gather_halo(parts):
        sides = []
        for side in range(2):
            a, b, c = (parts(side * 3 + j) for j in range(3))
            which = lax.broadcasted_iota(jnp.int32, a.shape, 1)
            sides.append(jnp.where(which < strip, a, jnp.where(which < 2 * strip, b, c)))
        return sides

    def line_tile(m, e, c, first):
        if e < REACH:
            buffer, at = up, SKIP + e * LINE
        elif e < REACH + rows:
            buffer, at = own, (e - REACH) * LINE
        else:
            buffer, at = dn, (e - REACH - rows) * LINE
        at += c * M + first
        return buffer[m, at : at + SUB, :]

    def halo_tile(m, side, c, first):
        at = c * M + first
        return halo[m, side, at : at + SUB, :]

    def real_part(a, b, x, y):
        return a * x + b * y

    def imag_part(a, b, x, y):
        return b * x - a * y

    def operands(tile, unit):
        lead = [tile(c, 0) for c in range(2)]
        if unit == 0:
            return lead, lead
        if 1 < unit <= SUB // 2:
            return lead, [pltpu.roll(v, SUB + 1 - unit, 0) for v in lead]
        if unit == 1:
            left, right = [], []
            for c in range(2):
                mid, late = tile(c, SUB // 2), tile(c, SUB - M + 5)
                left.append(jnp.where(sub < 4, lead[c], jnp.where(sub == 4, mid, late)))
                right.append(jnp.where(sub < 4, mid, jnp.where(sub == 4, tile(c, 5), late)))
            return left, right
        return lead, None

    def products(tile, row_tile, unit):
        (a, b), other = operands(tile, unit)
        if unit == 0:
            return a * a + b * b, None
        if other is None:
            image = M - 3 + unit - SUB // 2
            x, y = (jnp.broadcast_to(row_tile(c, image), (SUB, cols)) for c in range(2))
        else:
            x, y = other
        return real_part(a, b, x, y), imag_part(a, b, x, y)

    def tile_of(m, e):
        if e < lines_total:
            return functools.partial(line_tile, m, e)
        return functools.partial(halo_tile, m, e - lines_total)

    def row_of(m, e):
        tile = tile_of(m, e)
        return lambda c, image: tile(c, image)[0:1]

    def emit_side(unit, side, value, count):
        high, low = split(value)
        at = unit * 2 * SUB
        hbuf[at : at + 2 * SUB, side * cols : (side + 1) * cols] = high
        hbuf[count + at : count + at + 2 * SUB, side * cols : (side + 1) * cols] = low

    def edges(count):
        for r in range(0, rows, 2):
            band = w_halo[:, r * cols : (r + 2) * cols]
            value = jnp.dot(hbuf[0 : 2 * count], band, preferred_element_type=jnp.float32)
            value = value[0:count] + value[count:]
            ebuf[r, 0:count] = value[:, 0:cols]
            ebuf[r + 1, 0:count] = value[:, cols:]

    partials = {}
    for r in range(rows):
        partials.setdefault(own_range(r, rows), len(partials))

    def keep_own(unit, lines):
        for key, value in own_sums(lines, rows).items():
            at = (unit * len(partials) + partials[key]) * 2 * SUB
            pbuf[at : at + 2 * SUB, :] = value

    def emit_lines(unit, lines):
        def partial(r):
            at = (unit * len(partials) + partials[own_range(r, rows)]) * 2 * SUB
            return pbuf[at : at + 2 * SUB, :]

        for r, total in enumerate(window_sums(lines[:REACH], lines[REACH:], partial, rows)):
            high, low = split(total)
            ybuf[unit, r * 2 * SUB : (r + 1) * 2 * SUB, 0:cols] = high
            ybuf[unit, r * 2 * SUB : (r + 1) * 2 * SUB, cols:] = low

    def emit_main(unit, main, target, step, height=2 * SUB):
        for r in range(rows):
            at = r * step + unit * 2 * SUB
            target[at : at + height, :] = (
                main[r * 2 * SUB : r * 2 * SUB + height, :] + ebuf[r, unit * 2 * SUB : unit * 2 * SUB + height]
            )

    def both_halves(pair):
        first, second = pair
        return jnp.concatenate([first, jnp.zeros_like(first) if second is None else second], 0)

    own_lines = range(REACH, REACH + rows)
    far_lines = [*range(REACH), *range(REACH + rows, lines_total)]

    def fresh_values(m, e, unit):
        return both_halves(products(tile_of(m, e), row_of(m, e), unit))

    def fresh_own(m):
        for unit in range(len(GROUPS)):
            keep_own(unit, [fresh_values(m, e, unit) for e in own_lines])

    def fresh_sides(m):
        for side in range(2):
            for unit in range(len(GROUPS)):
                emit_side(unit, side, fresh_values(m, lines_total + side, unit), FRESH_ROWS)
        edges(FRESH_ROWS)

    def fresh_far(m):
        for unit in range(len(GROUPS)):
            emit_lines(unit, [fresh_values(m, e, unit) for e in far_lines])
            main = jnp.dot(ybuf[unit], w_main[...], preferred_element_type=jnp.float32)
            emit_main(unit, main, zbuf, FRESH_STEP, 2 * SUB if unit else SUB)

    def comp_row(e, c):
        if e < REACH:
            at = c * rows + rows - REACH + e
            return comp_up[at : at + 1, :]
        if e < REACH + rows:
            at = c * rows + e - REACH
            return comp_send[at : at + 1, :]
        if e < lines_total:
            at = c * rows + e - REACH - rows
            return comp_dn[at : at + 1, :]
        return chalo[e - lines_total, c : c + 1, :]

    def late_products(m, e, unit):
        tile = tile_of(m, e)
        x, y = (jnp.broadcast_to(comp_row(e, c), (SUB, cols)) for c in range(2))
        if unit == 0:
            a, b = tile(0, 0), tile(1, 0)
        else:
            a, b = (jnp.where(sub < 2 * SUB - M, v, tile(c, M - SUB)) for c, v in enumerate((x, y)))
        return jnp.concatenate([real_part(a, b, x, y), imag_part(a, b, x, y)], 0)

    def late_fields(m):
        for side in range(2):
            for unit in range(len(LATE)):
                emit_side(unit, side, late_products(m, lines_total + side, unit), LATE_ROWS)
        edges(LATE_ROWS)
        for unit in range(len(LATE)):
            emit_lines(unit, [late_products(m, e, unit) for e in far_lines])
        size = rows * 2 * SUB
        main = jnp.dot(
            ybuf[0 : len(LATE)].reshape(len(LATE) * size, 2 * cols), w_main[...], preferred_element_type=jnp.float32
        )
        for unit in range(len(LATE)):
            emit_main(unit, main[unit * size : (unit + 1) * size], zcbuf, LATE_STEP)

    def late_own(m):
        for unit in range(len(LATE)):
            keep_own(unit, [late_products(m, e, unit) for e in own_lines])

    def fresh_field(i, j, p):
        return zbuf[pl.ds(FIELDS[(i, j, p)], rows, stride=FRESH_STEP), :]

    def late_field(i, j, p):
        return zcbuf[pl.ds(LATE_FIELDS[(i, j, p)], rows, stride=LATE_STEP), :]

    class Coherence:
        def __init__(self):
            self.scales = {}
            self.slot = {}
            self.re = {}
            self.im = {}
            self.used = 0

        def keep(self, key, value):
            coh[self.used] = value
            self.slot[key] = self.used
            self.used += 1

        def get(self, key):
            return coh[self.slot[key]]

        def tally(self, sums, i, value, minus=False):
            if i in sums:
                sums[i] = sums[i] - value if minus else sums[i] + value
            else:
                sums[i] = -value if minus else value

        def add(self, images, pairs, field):
            for i in images:
                value = field(i, i, 0)
                scale = lax.rsqrt(jnp.maximum(value, covariance_floor))
                self.scales[i] = scale
                value = value * (scale * scale)
                self.keep((i, i), value)
                self.tally(self.re, i, value)
            for i, j in pairs:
                s = self.scales[i] * self.scales[j]
                c = field(i, j, 0) * s
                d = field(i, j, 1) * s
                self.keep((i, j, 0), c)
                self.keep((i, j, 1), c + d)
                self.keep((i, j, 2), c - d)
                self.tally(self.re, i, c)
                self.tally(self.re, j, c)
                self.tally(self.im, i, d)
                self.tally(self.im, j, d, True)

        def power(self):
            images = sorted(self.re)
            re = [self.re[i] for i in images]
            im = [self.im[i] for i in images]
            gain = None
            for step in range(ITERS):
                if step:
                    both = [x + y for x, y in zip(re, im)]
                    new_re, new_im = [], []
                    for i in images:
                        shared = first = second = None
                        for j in images:
                            if j == i:
                                continue
                            key = (i, j) if (i, j, 0) in self.slot else (j, i)
                            turn = key != (i, j)
                            c = self.get(key + (0,)) * both[j]
                            e = self.get(key + (2 if turn else 1,)) * im[j]
                            f = self.get(key + (1 if turn else 2,)) * re[j]
                            shared = c if shared is None else shared + c
                            first = e if first is None else first + e
                            second = f if second is None else second + f
                        c = self.get((i, i))
                        new_re.append((shared - first) + c * re[i])
                        new_im.append((shared - second) + c * im[i])
                    re, im = new_re, new_im
                squares = [x * x + y * y for x, y in zip(re, im)]
                while len(squares) > 1:
                    squares = [sum(squares[k + 1 : k + 2], squares[k]) for k in range(0, len(squares), 2)]
                square = squares[0] if gain is None else squares[0] * (gain * gain)
                inverse = lax.rsqrt(jnp.maximum(square, 1.0))
                gain = inverse if gain is None else gain * inverse
            return jnp.sqrt(square), gain, re, im

    def finish(m, number, length, gain, re, im):
        comp_re = comp_im = None
        for i in range(M):
            a = own[m, pl.ds(i, rows, stride=LINE), :]
            b = own[m, pl.ds(M + i, rows, stride=LINE), :]
            x = re[i] * a + im[i] * b
            y = re[i] * b - im[i] * a
            comp_re = x if comp_re is None else comp_re + x
            comp_im = y if comp_im is None else comp_im + y
        return comp_re * gain, comp_im * gain

    def put_linked(m, gain, re, im):
        factor = gain * mask
        for i in range(M):
            linked[m * M + i, 0] = re[i] * factor
            linked[m * M + i, 1] = im[i] * factor

    def share_of(number, length):
        return jnp.sum(mask * length, axis=0, keepdims=True) * (1.0 / number)

    def take_strips(m):
        each_around(lambda k: fresh_pair(m, k, False).wait_recv(), strips)
        for block in range(PACK // SUB):

            def turned(j, block=block):
                value = pack_recv[m, j]
                shift = (j % 3 - block) * strip % cols
                return pltpu.roll(value, shift, 1) if shift else value

            for side, value in enumerate(gather_halo(turned)):
                halo[m, side, block * SUB : (block + 1) * SUB, :] = value

    def take_beside(m):
        each_around(lambda k: fresh_pair(m, k, False).wait_recv(), beside)

    fresh_own(0)
    for m in range(1, MS):
        loads[1 + m].wait()
        place(m)
        pack(m)
    take_strips(0)
    for m in range(1, MS):
        each_around(lambda k, m=m: fresh_pair(m, k, True).start(), outward)
    fresh_sides(0)
    next_wave()
    take_beside(0)
    fresh_far(0)
    early = Coherence()
    early.add(range(M), PAIRS, fresh_field)
    length, gain, re, im = early.power()
    comp_re, comp_im = finish(0, M, length, gain, re, im)
    comp_send[0:rows, :] = comp_re
    comp_send[rows:, :] = comp_im

    def comp_pair(k, sending):
        dr, dc = AROUND[k]
        slot = mirror(k) if sending else k
        if dc == 0:
            source = comp_send
            target = comp_up if AROUND[slot][0] < 0 else comp_dn
        else:
            source = cpack_send.at[0 if dc < 0 else 1]
            target = cpack_recv.at[slot - 2]
        return pltpu.make_async_remote_copy(
            src_ref=source,
            dst_ref=target,
            send_sem=send_b.at[k],
            recv_sem=recv_b.at[slot],
            device_id=(my_row + dr, my_col + dc),
            device_id_type=mesh_id,
        )

    each_around(lambda k: comp_pair(k, True).start(), beside)
    for c, value in enumerate((comp_re, comp_im)):
        for side in range(2):
            total = jnp.zeros((rows, cols), jnp.float32)
            for copy in range(3):
                turned = pltpu.roll(value, REACH * side + strip * copy, 1, stride=REACH, stride_axis=0)
                first = strip * copy + sub * REACH
                total = jnp.where((lane >= first) & (lane < first + REACH), turned, total)
            cpack_send[side, c : c + 1, :] = jnp.sum(total, axis=0, keepdims=True)

    each_around(lambda k: comp_pair(k, True).start(), (2, 4, 5, 7, 3, 6))

    put_linked(0, gain, re, im)
    part[0:1] = share_of(M, length)
    last = MS - 1
    fresh_own(last)
    take_strips(last)
    fresh_sides(last)
    take_beside(last)
    fresh_far(last)
    late_own(last)
    joint = Coherence()
    joint.add(range(M), PAIRS, fresh_field)
    while len(pending) and pending[0][0] < len(offsets) - 1:
        next_wave()

    each_around(lambda k: comp_pair(k, False).wait_recv())
    for side, value in enumerate(gather_halo(lambda j: cpack_recv[j])):
        chalo[side] = value
    late_fields(last)
    joint.add([M], LATE_PAIRS, late_field)
    length, gain, re, im = joint.power()
    part[last : last + 1] = share_of(M + 1, length)
    while pending:
        next_wave()

    def reduce(count, me, device, source, buffer, sends, recvs):
        copies = []
        for step in range(1, count):
            copy = pltpu.make_async_remote_copy(
                src_ref=source,
                dst_ref=buffer.at[me],
                send_sem=sends.at[step],
                recv_sem=recvs.at[me],
                device_id=device(lax.rem(me + step, count)),
                device_id_type=mesh_id,
            )
            copy.start()
            copies.append(copy)
        buffer[me] = source[...]
        for step in range(1, count):
            other = lax.rem(me + step, count)
            pltpu.make_async_remote_copy(
                src_ref=source,
                dst_ref=buffer.at[other],
                send_sem=sends.at[step],
                recv_sem=recvs.at[other],
                device_id=device(other),
                device_id_type=mesh_id,
            ).wait_recv()
        for copy in copies:
            copy.wait_send()
        total = buffer[0]
        for other in range(1, count):
            total = total + buffer[other]
        return total

    def close_last():
        comp_re, comp_im = finish(last, M + 1, length, gain, re, im)
        comp_out[0] = comp_re
        comp_out[1] = comp_im
        put_linked(last, gain, re, im)

    def sent(k):
        dr, dc = AROUND[k]
        if dc == 0:
            source, target = own.at[:, pl.ds(0, EDGE)], up.at[:, pl.ds(0, EDGE)]
        else:
            source, target = pack_send.at[:, 0], pack_recv.at[:, 0]
        return pltpu.make_async_remote_copy(
            src_ref=source,
            dst_ref=target,
            send_sem=send_a.at[k],
            recv_sem=recv_a.at[0, k],
            device_id=(my_row + dr, my_col + dc),
            device_id_type=mesh_id,
        )

    def finish_sends():
        each_around(lambda k: sent(k).wait_send())
        each_around(lambda k: comp_pair(k, True).wait_send())

    def flips(position, count):
        steps = []
        size = 1
        while size < count:
            steps.append(size * (1 - 2 * lax.rem(position // size, 2)))
            size *= 2
        return steps

    def swapped(position, steps, mask_bits):
        for bit, step in enumerate(steps):
            if mask_bits >> bit & 1:
                position = position + step
        return position

    if direct:
        count = row_count * col_count
        row_steps, col_steps = flips(my_row, row_count), flips(my_col, col_count)

        def weight(code):
            return -bin(code // col_count).count("1") - code % col_count

        for code in sorted(range(1, count), key=weight):
            pltpu.make_async_remote_copy(
                src_ref=part,
                dst_ref=red_row.at[code],
                send_sem=send_r.at[0],
                recv_sem=recv_r.at[0],
                device_id=(
                    swapped(my_row, row_steps, code // col_count),
                    swapped(my_col, col_steps, code % col_count),
                ),
                device_id_type=mesh_id,
            ).start()
        close_last()
        finish_sends()
        everything = pltpu.make_async_remote_copy(
            src_ref=red_row.at[pl.ds(1, count - 1)],
            dst_ref=red_row.at[pl.ds(1, count - 1)],
            send_sem=send_r.at[0],
            recv_sem=recv_r.at[0],
            device_id=(swapped(my_row, row_steps, row_count - 1), swapped(my_col, col_steps, col_count - 1)),
            device_id_type=mesh_id,
        )
        everything.wait_recv()
        values = [part[...]] + [red_row[code] for code in range(1, count)]
        while len(values) > 1:
            values = [values[k] + values[k + 1] for k in range(0, len(values), 2)]
        total = values[0]
        strength[...] = total
        everything.wait_send()
    else:
        total = reduce(row_count, my_row, lambda d: (d, my_col), part, red_row, send_r, recv_r)
        part2 = red_col.at[col_count]
        part2[...] = total
        total = reduce(col_count, my_col, lambda d: (my_row, d), part2, red_col, send_r.at[pl.ds(row_count, col_count)], recv_r.at[pl.ds(row_count, col_count)])
        strength[...] = total
        close_last()
        finish_sends()


def closing(pixels, linked_in, comp_in, total, linked, comp, strength, scalars, sems):
    copies = [
        pltpu.make_async_copy(linked_in, linked, sems.at[0]),
        pltpu.make_async_copy(comp_in, comp, sems.at[1]),
        pltpu.make_async_copy(scalars, strength, sems.at[2]),
    ]
    for copy in copies[:2]:
        copy.start()
    sums = jnp.sum(total[...], axis=1, keepdims=True) * (1.0 / pixels)
    for m in range(MS):
        scalars[m] = sums[m, 0]
    copies[2].start()
    for copy in copies:
        copy.wait()


def shards(slc_stack, land_mask):
    rows, cols = land_mask.shape
    row_count, col_count = lax.axis_size("row"), lax.axis_size("col")
    f32, bf16 = jnp.float32, jnp.bfloat16
    vmem = pl.BlockSpec(memory_space=pltpu.VMEM)
    dma = pltpu.SemaphoreType.DMA
    hbm = pl.BlockSpec(memory_space=pltpu.HBM)
    devices = row_count * col_count
    direct = devices <= 64 and row_count & (row_count - 1) == 0 and col_count & (col_count - 1) == 0
    peers = devices if direct else row_count
    linked_shape = jax.ShapeDtypeStruct(slc_stack.shape, f32)
    comp_shape = jax.ShapeDtypeStruct((2, rows, cols), f32)
    linked, comp, total = pl.pallas_call(
        functools.partial(kernel, row_count, col_count, direct),
        out_shape=(linked_shape, comp_shape, jax.ShapeDtypeStruct((MS, cols), f32)),
        in_specs=[hbm, hbm],
        out_specs=(vmem, vmem, vmem),
        scratch_shapes=[
            pltpu.VMEM(slc_stack.shape, f32),
            pltpu.VMEM((rows, cols), jnp.int32),
            pltpu.VMEM((MS, rows * LINE + SUB, cols), f32),
            pltpu.VMEM((MS, EDGE + SUB, cols), f32),
            pltpu.VMEM((MS, EDGE + SUB, cols), f32),
            pltpu.VMEM((MS, 2, SUB, cols), f32),
            pltpu.VMEM((MS, 6, SUB, cols), f32),
            pltpu.VMEM((MS, 2, PACK, cols), f32),
            pltpu.VMEM((2 * rows, cols), f32),
            pltpu.VMEM((2 * rows, cols), f32),
            pltpu.VMEM((2 * rows, cols), f32),
            pltpu.VMEM((2, 2, cols), f32),
            pltpu.VMEM((6, 2, cols), f32),
            pltpu.VMEM((2, 2, cols), f32),
            pltpu.VMEM((2 * cols, cols), bf16),
            pltpu.VMEM((2 * cols, rows * cols), bf16),
            pltpu.VMEM((len(GROUPS) * rows * 2 * SUB, cols), f32),
            pltpu.VMEM((len(GROUPS), rows * 2 * SUB, 2 * cols), bf16),
            pltpu.VMEM((2 * FRESH_ROWS, 2 * cols), bf16),
            pltpu.VMEM((rows, FRESH_ROWS, cols), f32),
            pltpu.VMEM((rows * FRESH_STEP, cols), f32),
            pltpu.VMEM((rows * LATE_STEP, cols), f32),
            pltpu.VMEM((SLOTS, rows, cols), f32),
            pltpu.VMEM((MS, cols), f32),
            pltpu.VMEM((peers, MS, cols), f32),
            pltpu.VMEM((col_count + 1, MS, cols), f32),
            dma((MS + 1,)),
            pltpu.SemaphoreType.REGULAR((max(1, len(waves(row_count, col_count))),)),
            dma((len(AROUND),)),
            dma((MS, len(AROUND))),
            dma((len(AROUND),)),
            dma((len(AROUND),)),
            dma((1 if direct else row_count + col_count,)),
            dma((1 if direct else row_count + col_count,)),
        ],
        compiler_params=pltpu.CompilerParams(collective_id=0, has_side_effects=True, vmem_limit_bytes=16 << 20),
        name="linker",
    )(*(pltpu.with_memory_space_constraint(x, pltpu.HBM) for x in (slc_stack, land_mask)))
    return pl.pallas_call(
        functools.partial(closing, rows * cols * devices),
        out_shape=(linked_shape, comp_shape, jax.ShapeDtypeStruct((MS,), f32)),
        in_specs=[vmem, vmem, vmem],
        out_specs=(hbm, hbm, hbm),
        scratch_shapes=[pltpu.SMEM((MS,), f32), dma((3,))],
        compiler_params=pltpu.CompilerParams(vmem_limit_bytes=4 << 20),
        name="closing",
    )(linked, comp, total)


def solution(mesh):
    return jax.shard_map(
        shards,
        mesh=mesh,
        in_specs=(P(None, None, "row", "col"), P("row", "col")),
        out_specs=(P(None, None, "row", "col"), P(None, "row", "col"), P()),
        check_vma=False,
    )
```
